8 devices in a mesh: rep: 1 (over z), dp: 8 (over x, y, core).
Axes of the slice: x: 2, y: 2, z: 1, core: 2. Of those that a mesh axis runs over, the one named last changes fastest.
Arguments:
- g_w_gate: bfloat16 [8, 2, 896, 2560], P(('rep', 'dp'))
- g_w_up: bfloat16 [8, 2, 896, 2560], P(('rep', 'dp'))
- g_w_down: bfloat16 [8, 2, 2560, 896], P(('rep', 'dp'))
- w_gate: bfloat16 [2, 896, 2560], replicated
- w_up: bfloat16 [2, 896, 2560], replicated
- w_down: bfloat16 [2, 2560, 896], replicated
- m_w_gate: float32 [2, 896, 2560], P(None, 'dp')
- m_w_up: float32 [2, 896, 2560], P(None, 'dp')
- m_w_down: float32 [2, 2560, 896], P(None, 'dp')
- v_w_gate: float32 [2, 896, 2560], P(None, 'dp')
- v_w_up: float32 [2, 896, 2560], P(None, 'dp')
- v_w_down: float32 [2, 2560, 896], P(None, 'dp')
Outputs:
- output 1: bfloat16 [2, 896, 2560], P('rep')
- output 2: bfloat16 [2, 896, 2560], P('rep')
- output 3: bfloat16 [2, 2560, 896], P('rep')
- output 4: float32 [2, 896, 2560], P('rep', 'dp')
- output 5: float32 [2, 896, 2560], P('rep', 'dp')
- output 6: float32 [2, 2560, 896], P('rep', 'dp')
- output 7: float32 [2, 896, 2560], P('rep', 'dp')
- output 8: float32 [2, 896, 2560], P('rep', 'dp')
- output 9: float32 [2, 2560, 896], P('rep', 'dp')
All inputs are finite; a program needn't handle non-finite values.
Results may differ from the reference program's by a relative error of at most 0.022.
Values are sent between devices in bfloat16 or wider.
A program may use at most 2 GiB of HBM per device.

```python
import jax
import jax.numpy as jnp
from jax import lax

DEVICES = 8
D = 896
FF = 2560
LAYERS = 2
NAMES = ("w_gate", "w_up", "w_down")
SHAPES = {"w_gate": (LAYERS, D, FF), "w_up": (LAYERS, D, FF), "w_down": (LAYERS, FF, D)}


def setup_inputs(seed: int = 0, part: int = 0) -> dict:
    kz, *keys = jax.random.split(jax.random.key(seed), 1 + 5 * len(NAMES))
    loud = 2.0 ** jax.random.uniform(kz, (), jnp.float32, -1.0, 1.0)
    drawn = {}
    for name, key, both in zip(NAMES, keys[:3], keys[3:6], strict=True):
        own = jax.random.normal(jax.random.fold_in(key, part), (DEVICES, *SHAPES[name]), jnp.float32)
        shared = jax.random.normal(jax.random.fold_in(both, part), SHAPES[name], jnp.float32)
        drawn["g_" + name] = (loud * (0.7 * shared / DEVICES + 0.7 * own * DEVICES**-0.5)).astype(jnp.bfloat16)
    for name, key in zip(NAMES, keys[6:9], strict=True):
        drawn[name] = (jax.random.normal(key, SHAPES[name], jnp.float32) * SHAPES[name][1] ** -0.5).astype(jnp.bfloat16)
    for name, key in zip(NAMES, keys[9:12], strict=True):
        drawn["m_" + name] = loud * 0.5 * jax.random.normal(key, SHAPES[name], jnp.float32)
    for name, key in zip(NAMES, keys[12:15], strict=True):
        drawn["v_" + name] = loud * loud * jax.random.uniform(key, SHAPES[name], jnp.float32, 0.5, 1.5)
    return drawn


def adamw(w, m, v, g):
    m = 0.9 * m + 0.1 * g
    v = 0.95 * v + 0.05 * g * g
    step = m * lax.rsqrt(v + 1e-8) + 0.1 * w
    return (w - 0.02 * step).astype(jnp.bfloat16), m, v


def reference(g_w_gate, g_w_up, g_w_down, w_gate, w_up, w_down, m_w_gate, m_w_up, m_w_down, v_w_gate, v_w_up, v_w_down):
    def total(terms):
        return lax.scan(lambda so_far, term: (so_far + term.astype(jnp.float32), None), jnp.zeros(terms.shape[1:], jnp.float32), terms)[0]

    gradients = [total(terms).astype(jnp.bfloat16).astype(jnp.float32) for terms in (g_w_gate, g_w_up, g_w_down)]
    new = [
        adamw(w.astype(jnp.float32), m, v, g)
        for w, m, v, g in zip((w_gate, w_up, w_down), (m_w_gate, m_w_up, m_w_down), (v_w_gate, v_w_up, v_w_down), gradients, strict=True)
    ]
    return tuple(one[which] for which in range(3) for one in new)
```

```python
import functools

import jax
import jax.numpy as jnp
from jax import lax
from jax.experimental import pallas as pl
from jax.experimental.pallas import tpu as pltpu
from jax.sharding import PartitionSpec as P

MESH = pl.DeviceIdType.MESH
F32, BF16 = jnp.float32, jnp.bfloat16

LOAD, RS1, RS2, FETCH, STEP, STORED, AG1, AG2, END = range(9)
LAG = (0, 1, 3, 4, 5, 6, 7, 9, 10)
CHUNK = {112: 16, 320: 64}
PIECE = {112: (16, 512), 320: (16, 896)}


def adamw(w, m, v, g):
    m = 0.9 * m + 0.1 * g
    v = 0.95 * v + 0.05 * g * g
    step = m * lax.rsqrt(v + 1e-8) + 0.1 * w
    return (w - 0.02 * step).astype(BF16), m, v


def kinds():
    return {
        "far": (2, (2, 2), BF16),
        "near": (6, (2, 2), BF16),
        "partner": (None, (2, 2, 2), BF16),
        "send1": (3, (2, 2), BF16),
        "recv1": (None, (2, 2), BF16),
        "send2": (3, (2,), BF16),
        "recv2": (None, (2,), BF16),
        "w_in": (2, (2,), BF16),
        "m_in": (2, (2,), F32),
        "v_in": (2, (2,), F32),
        "m_out": (2, (2,), F32),
        "v_out": (2, (2,), F32),
    }


SEMS = ("far", "near", "partner", "partner_s", "recv1", "recv1_s", "recv2", "recv2_s", "fetch", "stored",
        "ag1", "ag2", "ag3", "own_s", "own3_s", "fwd_s", "fwd3_s")


def kernel(order, *refs):
    g, w, m, v = (refs[i : i + 3] for i in (0, 3, 6, 9))
    new_w, new_m, new_v = (refs[i : i + 3] for i in (12, 15, 18))
    refs = list(refs[21:])
    blocks = sorted({one.shape[1] for one in m})
    buf = {rows: {name: refs.pop(0) for name in kinds()} for rows in blocks}
    sem = {rows: {name: refs.pop(0) for name in SEMS} for rows in blocks}

    me = lax.axis_index("dp")
    x, y, core = me // 4, (me // 2) % 2, me % 2
    near_x, near_y, partner = me + 4 - 8 * x, me + 2 - 4 * y, me + 1 - 2 * core

    barrier = pltpu.get_barrier_semaphore()
    for other in (near_x, near_y, partner):
        pl.semaphore_signal(barrier, inc=1, device_id={"dp": other}, device_id_type=MESH)
    pl.semaphore_wait(barrier, 3)

    first, second = (near_x, near_y), (near_y, near_x)

    def block(layer, f, s, c):
        fx, fy = (f, s) if layer == 0 else (s, f)
        return (x + fx - 2 * x * fx) * 4 + (y + fy - 2 * y * fy) * 2 + c

    def run(stage, i, j):
        rows, cols = m[i].shape[1:]
        tall = CHUNK[rows]
        n = rows // tall
        b, sm = buf[rows], sem[rows]

        def at(layer, f, s, c=core):
            return (layer, pl.ds(pl.multiple_of(block(layer, f, s, c) * rows + j * tall, tall), tall))

        def slot(name):
            count = b[name].shape[0]
            return j if count == n else lax.rem(j, count)

        def of(name):
            return b[name].at[slot(name)]

        def take(name, like):
            pltpu.make_async_copy(of(like), of(like), sm[name].at[j]).wait()

        def local(src, dst, name):
            pltpu.make_async_copy(src, dst, sm[name].at[j]).start()

        def remote(src, dst, sent, received, other):
            pltpu.make_async_remote_copy(
                src_ref=src, dst_ref=dst, send_sem=sm[sent].at[j], recv_sem=sm[received].at[j],
                device_id={"dp": other}, device_id_type=MESH,
            ).start()

        def pieces(body):
            tr, tc = PIECE[rows]
            across = cols // tc

            def one(k, _):
                r = pl.multiple_of((k // across) * tr, tr)
                c = pl.multiple_of(lax.rem(k, across) * tc, 128)
                body(r, (pl.ds(r, tr), pl.ds(c, tc)), pl.ds(c, tc), tr)
                return 0

            lax.fori_loop(0, (tall // tr) * across, one, 0)

        own_rows = pl.ds(pl.multiple_of(j * tall, tall), tall)

        if stage == LOAD:
            for layer in (0, 1):
                for s in (0, 1):
                    remote(g[i].at[at(layer, 1, s, 1 - core)], of("partner").at[layer, 0, s], "partner_s", "partner", partner)
            for layer in (0, 1):
                for s in (0, 1):
                    local(g[i].at[at(layer, 1, s)], of("far").at[layer, s], "far")
            for layer in (0, 1):
                for s in (0, 1):
                    remote(g[i].at[at(layer, 0, s, 1 - core)], of("partner").at[layer, 1, s], "partner_s", "partner", partner)
                    local(g[i].at[at(layer, 0, s)], of("near").at[layer, s], "near")

        if stage == RS1:
            take("far", "far")
            take("partner", "partner")
            far, other, out = of("far"), of("partner"), of("send1")
            for layer in (0, 1):
                for s in (0, 1):
                    def add(r, p, c, tr, layer=layer, s=s):
                        out[(layer, s, *p)] = (far[(layer, s, *p)].astype(F32) + other[(layer, 0, s, *p)].astype(F32)).astype(BF16)
                    pieces(add)
            take("partner_s", "partner")
            for layer in (0, 1):
                remote(out.at[layer], of("recv1").at[layer], "recv1_s", "recv1", first[layer])

        if stage == RS2:
            take("near", "near")
            take("recv1", "recv1")
            near, other, came, out = of("near"), of("partner"), of("recv1"), of("send2")
            for layer in (0, 1):
                def add(r, p, c, tr, layer=layer):
                    out[(layer, *p)] = (
                        near[(layer, 1, *p)].astype(F32) + other[(layer, 1, 1, *p)].astype(F32) + came[(layer, 1, *p)].astype(F32)
                    ).astype(BF16)
                pieces(add)
            take("recv1_s", "recv1")
            for layer in (0, 1):
                remote(out.at[layer], of("recv2").at[layer], "recv2_s", "recv2", second[layer])

        if stage == FETCH:
            for layer in (0, 1):
                local(w[i].at[at(layer, 0, 0)], of("w_in").at[layer], "fetch")
                local(m[i].at[layer, own_rows], of("m_in").at[layer], "fetch")
                local(v[i].at[layer, own_rows], of("v_in").at[layer], "fetch")

        if stage == STEP:
            take("recv2", "recv2")
            take("fetch", "w_in")
            take("fetch", "m_in")
            take("fetch", "v_in")
            near, other, came, last = of("near"), of("partner"), of("recv1"), of("recv2")
            w_in, m_in, v_in, m_out, v_out = (of(k) for k in ("w_in", "m_in", "v_in", "m_out", "v_out"))
            for layer in (0, 1):
                start = block(layer, 0, 0, core) * rows + j * tall

                def step(r, p, c, tr, layer=layer, start=start):
                    total = near[(layer, 0, *p)].astype(F32) + other[(layer, 1, 0, *p)].astype(F32)
                    total = total + came[(layer, 0, *p)].astype(F32) + last[(layer, *p)].astype(F32)
                    total = total.astype(BF16).astype(F32)
                    one = adamw(w_in[(layer, *p)].astype(F32), m_in[(layer, *p)], v_in[(layer, *p)], total)
                    new_w[i][layer, pl.ds(pl.multiple_of(start + r, 16), tr), c] = one[0]
                    m_out[(layer, *p)] = one[1]
                    v_out[(layer, *p)] = one[2]
                pieces(step)
            take("recv2_s", "recv2")
            for layer in (0, 1):
                local(m_out.at[layer], new_m[i].at[layer, own_rows], "stored")
                local(v_out.at[layer], new_v[i].at[layer, own_rows], "stored")
            for layer in (0, 1):
                mine = new_w[i].at[at(layer, 0, 0)]
                remote(mine, mine, "own_s", "ag1", second[layer])
                remote(mine, mine, "own_s", "ag2", first[layer])
                remote(mine, mine, "own3_s", "ag3", partner)

        if stage == STORED:
            take("stored", "m_out")
            take("stored", "v_out")

        if stage == AG1:
            take("ag1", "recv2")
            for layer in (0, 1):
                came = new_w[i].at[at(layer, 0, 1)]
                remote(came, came, "fwd_s", "ag2", first[layer])
                remote(came, came, "fwd_s", "ag3", partner)

        if stage == AG2:
            take("ag2", "recv1")
            for layer in (0, 1):
                for s in (0, 1):
                    came = new_w[i].at[at(layer, 1, s)]
                    remote(came, came, "fwd3_s", "ag3", partner)

        if stage == END:
            take("ag3", "partner")
            take("own_s", "recv1")
            take("own3_s", "recv2")
            take("fwd_s", "recv1")
            take("fwd3_s", "recv1")

    spans, count = [], 0
    for i in order:
        n = m[i].shape[1] // CHUNK[m[i].shape[1]]
        spans.append((i, count, count + n))
        count += n

    def body(t, _):
        for stage in (END, LOAD, RS1, RS2, FETCH, STORED, STEP, AG1, AG2):
            u = t - LAG[stage]
            for i, start, end in spans:
                @pl.when(jnp.logical_and(u >= start, u < end))
                def _(i=i, start=start, stage=stage, u=u):
                    run(stage, i, u - start)
        return 0

    lax.fori_loop(0, count + LAG[END], body, 0)


def copy_out(n, *refs):
    sem = refs[2 * n]
    copies = [pltpu.make_async_copy(src, dst, sem.at[k]) for k, (src, dst) in enumerate(zip(refs[:n], refs[n : 2 * n], strict=True))]
    for copy in copies:
        copy.start()
    for copy in copies:
        copy.wait()


def to_hbm(*arrays):
    n = len(arrays)
    return pl.pallas_call(
        functools.partial(copy_out, n),
        out_shape=tuple(jax.ShapeDtypeStruct(a.shape, a.dtype) for a in arrays),
        in_specs=[pl.BlockSpec(memory_space=pl.ANY)] * n,
        out_specs=(pl.BlockSpec(memory_space=pl.ANY),) * n,
        scratch_shapes=[pltpu.SemaphoreType.DMA((n,))],
        compiler_params=pltpu.CompilerParams(vmem_limit_bytes=2**20),
    )(*arrays)


def solution(mesh):
    def step(*arrays):
        terms, weights, m, v = (arrays[i : i + 3] for i in (0, 3, 6, 9))
        scratch, sems = [], []
        for rows, cols in sorted({one.shape[1:] for one in m}):
            tall = CHUNK[rows]
            n = rows // tall
            for slots, held, kind in kinds().values():
                scratch.append(pltpu.VMEM((min(slots or n, n), *held, tall, cols), kind))
            sems += [pltpu.SemaphoreType.DMA((n,))] * len(SEMS)
        out = pl.pallas_call(
            functools.partial(kernel, (0, 2, 1)),
            out_shape=tuple(pltpu.VMEM(one.shape, one.dtype) for one in weights)
            + tuple(jax.ShapeDtypeStruct(one.shape, one.dtype) for one in (*m, *v)),
            in_specs=[pl.BlockSpec(memory_space=pl.ANY)] * 12,
            out_specs=(pl.BlockSpec(memory_space=pltpu.VMEM),) * 3 + (pl.BlockSpec(memory_space=pl.ANY),) * 6,
            scratch_shapes=scratch + sems,
            compiler_params=pltpu.CompilerParams(collective_id=0, has_side_effects=True, vmem_limit_bytes=35 * 2**20),
        )(*(t[0] for t in terms), *weights, *m, *v)
        return (*(to_hbm(one)[0] for one in out[:3]), *out[3:])

    all_of, cut = P(None, None, None), P(None, "dp", None)
    return jax.shard_map(
        step,
        mesh=mesh,
        in_specs=(P(("rep", "dp"), None, None, None),) * 3 + (all_of,) * 3 + (cut,) * 6,
        out_specs=(P("rep", None, None),) * 3 + (P("rep", "dp", None),) * 6,
        check_vma=False,
    )
```

```python
import functools

import jax
import jax.numpy as jnp
from jax import lax
from jax.experimental import pallas as pl
from jax.experimental.pallas import tpu as pltpu
from jax.sharding import PartitionSpec as P

MESH = pl.DeviceIdType.MESH
F32, BF16 = jnp.float32, jnp.bfloat16

LOAD, RS1, RS2, FETCH, STEP, AG1, AG2, END = range(8)
LAG = (0, 1, 3, 4, 5, 7, 9, 10)
CHUNK = {112: 16, 320: 32}
AHEAD = {"partner": 7, "recv1": 6, "recv2": 6}
PIECE = {112: (16, 512), 320: (16, 896)}


def adamw(w, m, v, g):
    m = 0.9 * m + 0.1 * g
    v = 0.95 * v + 0.05 * g * g
    step = m * lax.rsqrt(v + 1e-8) + 0.1 * w
    return (w - 0.02 * step).astype(BF16), m, v


def kinds():
    return {
        "far": (2, (2, 2), BF16),
        "near": (6, (2, 2), BF16),
        "partner": (AHEAD["partner"], (2, 2, 2), BF16),
        "send1": (3, (2, 2), BF16),
        "recv1": (AHEAD["recv1"], (2, 2), BF16),
        "send2": (3, (2,), BF16),
        "recv2": (AHEAD["recv2"], (2,), BF16),
        "w_in": (2, (2,), BF16),
        "m_in": (2, (2,), F32),
        "v_in": (2, (2,), F32),
    }


SEMS = ("far", "near", "partner", "partner_s", "recv1", "recv1_s", "recv2", "recv2_s", "fetch",
        "ag1", "ag2", "ag3", "own_s", "own3_s", "fwd_s", "fwd3_s")


def kernel(order, *refs):
    g, w, m, v = (refs[i : i + 3] for i in (0, 3, 6, 9))
    new_w, new_m, new_v = (refs[i : i + 3] for i in (12, 15, 18))
    refs = list(refs[21:])
    blocks = sorted({one.shape[1] for one in m})
    buf = {rows: {name: refs.pop(0) for name in kinds()} for rows in blocks}
    sem = {rows: {name: refs.pop(0) for name in SEMS} for rows in blocks}
    credit = refs.pop(0)
    total = sum(one.shape[1] // CHUNK[one.shape[1]] for one in m)

    me = lax.axis_index("dp")
    x, y, core = me // 4, (me // 2) % 2, me % 2
    near_x, near_y, partner = me + 4 - 8 * x, me + 2 - 4 * y, me + 1 - 2 * core

    barrier = pltpu.get_barrier_semaphore()
    for other in (near_x, near_y, partner):
        pl.semaphore_signal(barrier, inc=1, device_id={"dp": other}, device_id_type=MESH)
    pl.semaphore_wait(barrier, 3)

    first, second = (near_x, near_y), (near_y, near_x)

    def block(layer, f, s, c):
        fx, fy = (f, s) if layer == 0 else (s, f)
        return (x + fx - 2 * x * fx) * 4 + (y + fy - 2 * y * fy) * 2 + c

    def give(u, name, others):
        @pl.when(u + AHEAD[name] < total)
        def _():
            for k, other in others:
                pl.semaphore_signal(credit.at[k], inc=1, device_id={"dp": other}, device_id_type=MESH)

    def spend(u, name, ks):
        @pl.when(u >= AHEAD[name])
        def _():
            for k in ks:
                pl.semaphore_wait(credit.at[k], 1)

    def run(stage, i, j, u):
        rows, cols = m[i].shape[1:]
        tall = CHUNK[rows]
        n = rows // tall
        b, sm = buf[rows], sem[rows]

        def at(layer, f, s, c=core):
            return (layer, pl.ds(pl.multiple_of(block(layer, f, s, c) * rows + j * tall, tall), tall))

        def slot(name):
            count = b[name].shape[0]
            return j if count == n else lax.rem(j, count)

        def of(name):
            return b[name].at[slot(name)]

        def take(name, like):
            pltpu.make_async_copy(of(like), of(like), sm[name].at[j]).wait()

        def local(src, dst, name):
            pltpu.make_async_copy(src, dst, sm[name].at[j]).start()

        def remote(src, dst, sent, received, other):
            pltpu.make_async_remote_copy(
                src_ref=src, dst_ref=dst, send_sem=sm[sent].at[j], recv_sem=sm[received].at[j],
                device_id={"dp": other}, device_id_type=MESH,
            ).start()

        def pieces(body):
            tr, tc = PIECE[rows]
            across = cols // tc

            def one(k, _):
                r = pl.multiple_of((k // across) * tr, tr)
                c = pl.multiple_of(lax.rem(k, across) * tc, 128)
                body(r, (pl.ds(r, tr), pl.ds(c, tc)), pl.ds(c, tc), tr)
                return 0

            lax.fori_loop(0, (tall // tr) * across, one, 0)

        own_rows = pl.ds(pl.multiple_of(j * tall, tall), tall)

        if stage == LOAD:
            spend(u, "partner", (0,))
            for layer in (0, 1):
                for s in (0, 1):
                    remote(g[i].at[at(layer, 1, s, 1 - core)], of("partner").at[layer, 0, s], "partner_s", "partner", partner)
            for layer in (0, 1):
                for s in (0, 1):
                    local(g[i].at[at(layer, 1, s)], of("far").at[layer, s], "far")
            for layer in (0, 1):
                for s in (0, 1):
                    remote(g[i].at[at(layer, 0, s, 1 - core)], of("partner").at[layer, 1, s], "partner_s", "partner", partner)
                    local(g[i].at[at(layer, 0, s)], of("near").at[layer, s], "near")

        if stage == RS1:
            take("far", "far")
            take("partner", "partner")
            far, other, out = of("far"), of("partner"), of("send1")
            for layer in (0, 1):
                for s in (0, 1):
                    def add(r, p, c, tr, layer=layer, s=s):
                        out[(layer, s, *p)] = (far[(layer, s, *p)].astype(F32) + other[(layer, 0, s, *p)].astype(F32)).astype(BF16)
                    pieces(add)
            take("partner_s", "partner")
            spend(u, "recv1", (1, 2))
            for layer in (0, 1):
                remote(out.at[layer], of("recv1").at[layer], "recv1_s", "recv1", first[layer])

        if stage == RS2:
            take("near", "near")
            take("recv1", "recv1")
            near, other, came, out = of("near"), of("partner"), of("recv1"), of("send2")
            for layer in (0, 1):
                def add(r, p, c, tr, layer=layer):
                    out[(layer, *p)] = (
                        near[(layer, 1, *p)].astype(F32) + other[(layer, 1, 1, *p)].astype(F32) + came[(layer, 1, *p)].astype(F32)
                    ).astype(BF16)
                pieces(add)
            take("recv1_s", "recv1")
            for layer in (0, 1):
                remote(out.at[layer], of("recv2").at[layer], "recv2_s", "recv2", second[layer])

        if stage == FETCH:
            for layer in (0, 1):
                local(w[i].at[at(layer, 0, 0)], of("w_in").at[layer], "fetch")
                local(m[i].at[layer, own_rows], of("m_in").at[layer], "fetch")
                local(v[i].at[layer, own_rows], of("v_in").at[layer], "fetch")

        if stage == STEP:
            take("recv2", "recv2")
            take("fetch", "w_in")
            take("fetch", "m_in")
            take("fetch", "v_in")
            near, other, came, last = of("near"), of("partner"), of("recv1"), of("recv2")
            w_in, m_in, v_in = (of(k) for k in ("w_in", "m_in", "v_in"))
            for layer in (0, 1):
                start = block(layer, 0, 0, core) * rows + j * tall

                def step(r, p, c, tr, layer=layer, start=start):
                    gsum = near[(layer, 0, *p)].astype(F32) + other[(layer, 1, 0, *p)].astype(F32)
                    gsum = gsum + came[(layer, 0, *p)].astype(F32) + last[(layer, *p)].astype(F32)
                    gsum = gsum.astype(BF16).astype(F32)
                    one = adamw(w_in[(layer, *p)].astype(F32), m_in[(layer, *p)], v_in[(layer, *p)], gsum)
                    new_w[i][layer, pl.ds(pl.multiple_of(start + r, 16), tr), c] = one[0]
                    here = pl.ds(pl.multiple_of(j * tall + r, 16), tr)
                    new_m[i][layer, here, c] = one[1]
                    new_v[i][layer, here, c] = one[2]
                pieces(step)
            take("recv2_s", "recv2")
            give(u, "partner", ((0, partner),))
            give(u, "recv1", ((1, near_x), (2, near_y)))
            for layer in (0, 1):
                mine = new_w[i].at[at(layer, 0, 0)]
                remote(mine, mine, "own_s", "ag1", second[layer])
                remote(mine, mine, "own_s", "ag2", first[layer])
                remote(mine, mine, "own3_s", "ag3", partner)

        if stage == AG1:
            take("ag1", "recv2")
            for layer in (0, 1):
                came = new_w[i].at[at(layer, 0, 1)]
                remote(came, came, "fwd_s", "ag2", first[layer])
                remote(came, came, "fwd_s", "ag3", partner)

        if stage == AG2:
            take("ag2", "recv1")
            for layer in (0, 1):
                for s in (0, 1):
                    came = new_w[i].at[at(layer, 1, s)]
                    remote(came, came, "fwd3_s", "ag3", partner)

        if stage == END:
            take("ag3", "partner")
            take("own_s", "recv1")
            take("own3_s", "recv2")
            take("fwd_s", "recv1")
            take("fwd3_s", "recv1")

    spans, count = [], 0
    for i in order:
        n = m[i].shape[1] // CHUNK[m[i].shape[1]]
        spans.append((i, count, count + n))
        count += n

    def body(t, _):
        for stage in (END, LOAD, RS1, RS2, FETCH, STEP, AG1, AG2):
            u = t - LAG[stage]
            for i, start, end in spans:
                @pl.when(jnp.logical_and(u >= start, u < end))
                def _(i=i, start=start, stage=stage, u=u):
                    run(stage, i, u - start, u)
        return 0

    lax.fori_loop(0, count + LAG[END], body, 0)


def copy_out(n, *refs):
    sem = refs[2 * n]
    copies = [pltpu.make_async_copy(src, dst, sem.at[k]) for k, (src, dst) in enumerate(zip(refs[:n], refs[n : 2 * n], strict=True))]
    for copy in copies:
        copy.start()
    for copy in copies:
        copy.wait()


def to_hbm(*arrays):
    n = len(arrays)
    return pl.pallas_call(
        functools.partial(copy_out, n),
        out_shape=tuple(jax.ShapeDtypeStruct(a.shape, a.dtype) for a in arrays),
        in_specs=[pl.BlockSpec(memory_space=pl.ANY)] * n,
        out_specs=(pl.BlockSpec(memory_space=pl.ANY),) * n,
        scratch_shapes=[pltpu.SemaphoreType.DMA((n,))],
        compiler_params=pltpu.CompilerParams(vmem_limit_bytes=2**20),
    )(*arrays)


def solution(mesh):
    def step(*arrays):
        terms, weights, m, v = (arrays[i : i + 3] for i in (0, 3, 6, 9))
        scratch, sems = [], []
        for rows, cols in sorted({one.shape[1:] for one in m}):
            tall = CHUNK[rows]
            n = rows // tall
            for slots, held, kind in kinds().values():
                scratch.append(pltpu.VMEM((min(slots or n, n), *held, tall, cols), kind))
            sems += [pltpu.SemaphoreType.DMA((n,))] * len(SEMS)
        out = pl.pallas_call(
            functools.partial(kernel, (0, 2, 1)),
            out_shape=tuple(pltpu.VMEM(one.shape, one.dtype) for one in (*weights, *m, *v)),
            in_specs=[pl.BlockSpec(memory_space=pl.ANY)] * 12,
            out_specs=(pl.BlockSpec(memory_space=pltpu.VMEM),) * 9,
            scratch_shapes=[*scratch, *sems, pltpu.SemaphoreType.REGULAR((3,))],
            compiler_params=pltpu.CompilerParams(collective_id=0, has_side_effects=True, vmem_limit_bytes=22 * 2**20),
        )(*(t[0] for t in terms), *weights, *m, *v)
        first, rest = to_hbm(*out[:2]), to_hbm(*out[2:])
        return (*first, *rest)

    all_of, cut = P(None, None, None), P(None, "dp", None)
    return jax.shard_map(
        step,
        mesh=mesh,
        in_specs=(P(("rep", "dp"), None, None, None),) * 3 + (all_of,) * 3 + (cut,) * 6,
        out_specs=(P("rep", None, None),) * 3 + (P("rep", "dp", None),) * 6,
        check_vma=False,
    )
```

```python
import functools

import jax
import jax.numpy as jnp
from jax import lax
from jax.experimental import pallas as pl
from jax.experimental.pallas import tpu as pltpu
from jax.sharding import PartitionSpec as P

MESH = pl.DeviceIdType.MESH
F32, BF16 = jnp.float32, jnp.bfloat16

LOAD, RS1, RS2, FETCH, STEP, AG1, AG2, END = range(8)
LAG = (0, 1, 3, 4, 5, 7, 9, 10)
ORDER = (END, LOAD, RS1, RS2, FETCH, STEP, AG1, AG2)
RUNS = ((2, 0, 1, 1), (0, 0, 1, 1), (1, 0, 1, 1))
CHUNK = {2560: 16, 896: 32}
AHEAD = {"partner": 7, "recv1": 6, "recv2": 6}
WIDE = 512

BUFFERS = {
    "far": (2, (2, 2), BF16),
    "near": (6, (2, 2), BF16),
    "partner": (AHEAD["partner"], (2, 2, 2), BF16),
    "send1": (3, (2, 2), BF16),
    "recv1": (AHEAD["recv1"], (2, 2), BF16),
    "send2": (3, (2,), BF16),
    "recv2": (AHEAD["recv2"], (2,), BF16),
    "w_in": (2, (2,), BF16),
    "m_in": (2, (2,), F32),
    "v_in": (2, (2,), F32),
}
SEMS = {"far": 7, "near": 7, "sent1": 4, "recv1": 6, "recv2": 6, "sent2": 3, "ag1": 5, "ag2": 9, "ag3": 10, "sent3": 5}


def adamw(w, m, v, g):
    m = 0.9 * m + 0.1 * g
    v = 0.95 * v + 0.05 * g * g
    step = m * lax.rsqrt(v + 1e-8) + 0.1 * w
    return (w - 0.02 * step).astype(BF16), m, v


def kernel(*refs):
    g, w, m, v = (refs[i : i + 3] for i in (0, 3, 6, 9))
    new_w, new_m, new_v = (refs[i : i + 3] for i in (12, 15, 18))
    refs = list(refs[21:])
    widths = sorted({one.shape[2] for one in m})
    buf = {cols: {name: refs.pop(0) for name in BUFFERS} for cols in widths}
    sem = {name: refs.pop(0) for name in SEMS}
    credit = refs.pop(0)

    spans, total, done = [], 0, dict.fromkeys(widths, 0)
    for i, start, end, parts in RUNS:
        rows, cols = m[i].shape[1:]
        n = rows // CHUNK[cols]
        a, b = n * start // parts, n * end // parts
        spans.append((i, total, total + b - a, a, done[cols]))
        total += b - a
        done[cols] += b - a

    me = lax.axis_index("dp")
    x, y, core = me // 4, (me // 2) % 2, me % 2
    near_x, near_y, partner = me + 4 - 8 * x, me + 2 - 4 * y, me + 1 - 2 * core
    first, second = (near_x, near_y), (near_y, near_x)

    barrier = pltpu.get_barrier_semaphore()
    for other in (partner, near_x, near_y):
        pl.semaphore_signal(barrier, inc=1, device_id={"dp": other}, device_id_type=MESH)
    pl.semaphore_wait(barrier, 3)

    def block(layer, f, s, c):
        fx, fy = (f, s) if layer == 0 else (s, f)
        return (x + fx - 2 * x * fx) * 4 + (y + fy - 2 * y * fy) * 2 + c

    def give(u, name, others):
        @pl.when(u + AHEAD[name] < total)
        def _():
            for k, other in others:
                pl.semaphore_signal(credit.at[k], inc=1, device_id={"dp": other}, device_id_type=MESH)

    def spend(u, name, ks):
        @pl.when(u >= AHEAD[name])
        def _():
            for k in ks:
                pl.semaphore_wait(credit.at[k], 1)

    def run(stage, i, j, u, pos):
        rows, cols = m[i].shape[1:]
        b = buf[cols]
        wide = WIDE if cols % WIDE == 0 else cols
        tall = CHUNK[cols]

        def at(layer, f, s, c=core):
            return (layer, pl.ds(pl.multiple_of(block(layer, f, s, c) * rows + j * tall, tall), tall))

        def of(name):
            return b[name].at[lax.rem(pos, b[name].shape[0])]

        def signal(name):
            return sem[name].at[lax.rem(u, sem[name].shape[0])]

        def take(name, chunks):
            like = g[i].at[0, pl.ds(0, chunks * tall)]
            pltpu.make_async_copy(like, like, signal(name)).wait()

        def local(src, dst, name):
            pltpu.make_async_copy(src, dst, signal(name)).start()

        def remote(src, dst, sent, received, other):
            pltpu.make_async_remote_copy(
                src_ref=src, dst_ref=dst, send_sem=signal(sent), recv_sem=signal(received),
                device_id={"dp": other}, device_id_type=MESH,
            ).start()

        def pieces(body):
            def one(k, _):
                body((slice(None), pl.ds(pl.multiple_of(k * wide, 128), wide)))
                return 0

            lax.fori_loop(0, cols // wide, one, 0)

        own = pl.ds(pl.multiple_of(j * tall, tall), tall)
        other = of("partner")

        if stage == LOAD:
            spend(u, "partner", (0,))
            for side, mine in ((1, "far"), (0, "near")):
                for layer in (0, 1):
                    for s in (0, 1):
                        remote(g[i].at[at(layer, side, s, 1 - core)], other.at[1 - side, layer, s], "sent1", mine, partner)
                for layer in (0, 1):
                    for s in (0, 1):
                        local(g[i].at[at(layer, side, s)], of(mine).at[layer, s], mine)

        if stage == RS1:
            far, out = of("far"), of("send1")
            take("far", 8)
            for layer in (0, 1):
                for s in (0, 1):
                    def add(p, layer=layer, s=s):
                        out[(layer, s, *p)] = (far[(layer, s, *p)].astype(F32) + other[(0, layer, s, *p)].astype(F32)).astype(BF16)
                    pieces(add)
            spend(u, "recv1", (1, 2))
            for layer in (0, 1):
                remote(out.at[layer], of("recv1").at[layer], "sent1", "recv1", first[layer])

        if stage == RS2:
            near, came, out = of("near"), of("recv1"), of("send2")
            take("near", 8)
            take("recv1", 4)
            for layer in (0, 1):
                def add(p, layer=layer):
                    out[(layer, *p)] = (
                        near[(layer, 1, *p)].astype(F32) + other[(1, layer, 1, *p)].astype(F32) + came[(layer, 1, *p)].astype(F32)
                    ).astype(BF16)
                pieces(add)
            take("sent1", 12)
            for layer in (0, 1):
                remote(out.at[layer], of("recv2").at[layer], "sent2", "recv2", second[layer])

        if stage == FETCH:
            for layer in (0, 1):
                local(w[i].at[at(layer, 0, 0)], of("w_in").at[layer], "recv2")
                local(m[i].at[layer, own], of("m_in").at[layer], "recv2")
                local(v[i].at[layer, own], of("v_in").at[layer], "recv2")

        if stage == STEP:
            near, came, last = of("near"), of("recv1"), of("recv2")
            w_in, m_in, v_in = of("w_in"), of("m_in"), of("v_in")
            take("recv2", 12)
            for layer in (0, 1):
                rows_of = at(layer, 0, 0)[1]

                def step(p, layer=layer, rows_of=rows_of):
                    gsum = near[(layer, 0, *p)].astype(F32) + other[(1, layer, 0, *p)].astype(F32)
                    gsum = gsum + came[(layer, 0, *p)].astype(F32) + last[(layer, *p)].astype(F32)
                    gsum = gsum.astype(BF16).astype(F32)
                    one = adamw(w_in[(layer, *p)].astype(F32), m_in[(layer, *p)], v_in[(layer, *p)], gsum)
                    new_w[i][layer, rows_of, p[1]] = one[0]
                    new_m[i][layer, own, p[1]] = one[1]
                    new_v[i][layer, own, p[1]] = one[2]
                pieces(step)
            take("sent2", 2)
            give(u, "partner", ((0, partner),))
            give(u, "recv1", ((1, near_x), (2, near_y)))
            for layer in (0, 1):
                mine = new_w[i].at[at(layer, 0, 0)]
                remote(mine, mine, "sent3", "ag1", second[layer])
                remote(mine, mine, "sent3", "ag2", first[layer])
                remote(mine, mine, "sent3", "ag3", partner)

        if stage == AG1:
            take("ag1", 2)
            for layer in (0, 1):
                came = new_w[i].at[at(layer, 0, 1)]
                remote(came, came, "sent3", "ag2", first[layer])
            for layer in (0, 1):
                came = new_w[i].at[at(layer, 0, 1)]
                remote(came, came, "sent3", "ag3", partner)

        if stage == AG2:
            take("ag2", 4)
            for layer in (0, 1):
                for s in (0, 1):
                    came = new_w[i].at[at(layer, 1, s)]
                    remote(came, came, "sent3", "ag3", partner)

        if stage == END:
            take("ag3", 8)
            take("sent3", 14)

    def body(t, _):
        for stage in ORDER:
            u = t - LAG[stage]
            for i, start, end, chunk, pos in spans:
                @pl.when(jnp.logical_and(u >= start, u < end))
                def _(i=i, start=start, chunk=chunk, pos=pos, stage=stage, u=u):
                    run(stage, i, u - start + chunk, u, u - start + pos)
        return 0

    lax.fori_loop(0, total + LAG[END], body, 0)


def copy_out(n, *refs):
    copies = [
        pltpu.make_async_copy(src.at[layer], dst.at[layer], refs[2 * n])
        for src, dst in zip(refs[:n], refs[n : 2 * n], strict=True) for layer in (0, 1)
    ]
    for copy in copies:
        copy.start()
    for copy in copies:
        copy.wait()


def to_hbm(*arrays):
    n = len(arrays)
    return pl.pallas_call(
        functools.partial(copy_out, n),
        out_shape=tuple(jax.ShapeDtypeStruct(a.shape, a.dtype) for a in arrays),
        in_specs=[pl.BlockSpec(memory_space=pl.ANY)] * n,
        out_specs=(pl.BlockSpec(memory_space=pl.ANY),) * n,
        scratch_shapes=[pltpu.SemaphoreType.DMA],
        compiler_params=pltpu.CompilerParams(vmem_limit_bytes=2**20),
    )(*arrays)


def solution(mesh):
    def step(*arrays):
        terms, weights, m, v = (arrays[i : i + 3] for i in (0, 3, 6, 9))
        widths = sorted({one.shape[2] for one in m})
        scratch = [pltpu.VMEM((slots, *held, CHUNK[cols], cols), kind) for cols in widths for slots, held, kind in BUFFERS.values()]
        sems = [pltpu.SemaphoreType.DMA((slots,)) for slots in SEMS.values()]
        out = pl.pallas_call(
            kernel,
            out_shape=tuple(pltpu.VMEM(one.shape, one.dtype) for one in (*weights, *m, *v)),
            in_specs=[pl.BlockSpec(memory_space=pl.ANY)] * 12,
            out_specs=(pl.BlockSpec(memory_space=pltpu.VMEM),) * 9,
            scratch_shapes=[*scratch, *sems, pltpu.SemaphoreType.REGULAR((3,))],
            compiler_params=pltpu.CompilerParams(collective_id=0, has_side_effects=True, vmem_limit_bytes=22 * 2**20),
        )(*(t[0] for t in terms), *weights, *m, *v)
        return (*to_hbm(*out[:2]), *to_hbm(*out[2:]))

    all_of, cut = P(None, None, None), P(None, "dp", None)
    return jax.shard_map(
        step,
        mesh=mesh,
        in_specs=(P(("rep", "dp"), None, None, None),) * 3 + (all_of,) * 3 + (cut,) * 6,
        out_specs=(P("rep", None, None),) * 3 + (P("rep", "dp", None),) * 6,
        check_vma=False,
    )
```

```python
import functools

import jax
import jax.numpy as jnp
from jax import lax
from jax.experimental import pallas as pl
from jax.experimental.pallas import tpu as pltpu
from jax.sharding import PartitionSpec as P

MESH = pl.DeviceIdType.MESH
F32, BF16 = jnp.float32, jnp.bfloat16

LOAD, RS1, RS2, FETCH, STEP, AG1, AG2, END = range(8)
LAG = (0, 1, 3, 4, 5, 7, 9, 10)
ORDER = (END, LOAD, RS1, RS2, FETCH, STEP, AG1, AG2)
RUNS = ((2, 0, 1, 1), (1, 0, 1, 1), (0, 0, 1, 1))
APART = 1
CHUNK = {2560: 16, 896: 32}
AHEAD = {"partner": 7, "recv1": 6, "recv2": 6}
WIDE = 512

BUFFERS = {
    "far": (2, (2, 2), BF16),
    "near": (6, (2, 2), BF16),
    "partner": (AHEAD["partner"], (2, 2, 2), BF16),
    "send1": (3, (2, 2), BF16),
    "recv1": (AHEAD["recv1"], (2, 2), BF16),
    "send2": (3, (2,), BF16),
    "recv2": (AHEAD["recv2"], (2,), BF16),
    "w_in": (4, (2,), BF16),
    "m_in": (2, (2,), F32),
    "v_in": (2, (2,), F32),
}
SEMS = {"far": 7, "near": 7, "sent1": 4, "recv1": 6, "recv2": 6, "sent2": 3, "ag1": 5, "ag2": 9, "ag3": 10, "sent3": 5}


def adamw(w, m, v, g):
    m = 0.9 * m + 0.1 * g
    v = 0.95 * v + 0.05 * g * g
    step = m * lax.rsqrt(v + 1e-8) + 0.1 * w
    return (w - 0.02 * step).astype(BF16), m, v


def kernel(*refs):
    g, w, m, v = (refs[i : i + 3] for i in (0, 3, 6, 9))
    new_w, new_m, new_v = (refs[i : i + 3] for i in (12, 15, 18))
    refs = list(refs[21:])
    widths = sorted({one.shape[2] for one in m})
    buf = {cols: {name: refs.pop(0) for name in BUFFERS} for cols in widths}
    sem = {name: refs.pop(0) for name in SEMS}
    credit = refs.pop(0)

    spans, total, done = [], 0, dict.fromkeys(widths, 0)
    for i, start, end, parts in RUNS:
        rows, cols = m[i].shape[1:]
        n = rows // CHUNK[cols]
        a, b = n * start // parts, n * end // parts
        spans.append((i, total, total + b - a, a, done[cols]))
        total += b - a
        done[cols] += b - a

    me = lax.axis_index("dp")
    x, y, core = me // 4, (me // 2) % 2, me % 2
    near_x, near_y, partner = me + 4 - 8 * x, me + 2 - 4 * y, me + 1 - 2 * core
    first, second = (near_x, near_y), (near_y, near_x)

    barrier = pltpu.get_barrier_semaphore()
    for other in (partner, near_x, near_y):
        pl.semaphore_signal(barrier, inc=1, device_id={"dp": other}, device_id_type=MESH)
    pl.semaphore_wait(barrier, 3)

    def block(layer, f, s, c):
        fx, fy = (f, s) if layer == 0 else (s, f)
        return (x + fx - 2 * x * fx) * 4 + (y + fy - 2 * y * fy) * 2 + c

    def give(u, name, others):
        @pl.when(u + AHEAD[name] < total)
        def _():
            for k, other in others:
                pl.semaphore_signal(credit.at[k], inc=1, device_id={"dp": other}, device_id_type=MESH)

    def spend(u, name, ks):
        @pl.when(u >= AHEAD[name])
        def _():
            for k in ks:
                pl.semaphore_wait(credit.at[k], 1)

    def run(stage, i, j, u, pos):
        rows, cols = m[i].shape[1:]
        b = buf[cols]
        wide = WIDE if cols % WIDE == 0 else cols
        tall = CHUNK[cols]

        def at(layer, f, s, c=core):
            return (layer, pl.ds(pl.multiple_of(block(layer, f, s, c) * rows + j * tall, tall), tall))

        def of(name):
            return b[name].at[lax.rem(pos, b[name].shape[0])]

        def signal(name):
            return sem[name].at[lax.rem(u, sem[name].shape[0])]

        def take(name, chunks):
            like = g[i].at[0, pl.ds(0, chunks * tall)]
            pltpu.make_async_copy(like, like, signal(name)).wait()

        def local(src, dst, name):
            pltpu.make_async_copy(src, dst, signal(name)).start()

        def remote(src, dst, sent, received, other):
            pltpu.make_async_remote_copy(
                src_ref=src, dst_ref=dst, send_sem=signal(sent), recv_sem=signal(received),
                device_id={"dp": other}, device_id_type=MESH,
            ).start()

        def pieces(body):
            def one(k, _):
                body((slice(None), pl.ds(pl.multiple_of(k * wide, 128), wide)))
                return 0

            lax.fori_loop(0, cols // wide, one, 0)

        own = pl.ds(pl.multiple_of(j * tall, tall), tall)
        other = of("partner")

        if stage == LOAD:
            spend(u, "partner", (0,))
            for side, mine in ((1, "far"), (0, "near")):
                for layer in (0, 1):
                    for s in (0, 1):
                        remote(g[i].at[at(layer, side, s, 1 - core)], other.at[1 - side, layer, s], "sent1", mine, partner)
                for layer in (0, 1):
                    for s in (0, 1):
                        local(g[i].at[at(layer, side, s)], of(mine).at[layer, s], mine)

        if stage == RS1:
            far, out = of("far"), of("send1")
            take("far", 8)
            for layer in (0, 1):
                for s in (0, 1):
                    def add(p, layer=layer, s=s):
                        out[(layer, s, *p)] = (far[(layer, s, *p)].astype(F32) + other[(0, layer, s, *p)].astype(F32)).astype(BF16)
                    pieces(add)
            spend(u, "recv1", (1, 2))
            for layer in (0, 1):
                remote(out.at[layer], of("recv1").at[layer], "sent1", "recv1", first[layer])

        if stage == RS2:
            near, came, out = of("near"), of("recv1"), of("send2")
            take("near", 8)
            take("recv1", 4)
            for layer in (0, 1):
                def add(p, layer=layer):
                    out[(layer, *p)] = (
                        near[(layer, 1, *p)].astype(F32) + other[(1, layer, 1, *p)].astype(F32) + came[(layer, 1, *p)].astype(F32)
                    ).astype(BF16)
                pieces(add)
            take("sent1", 12)
            for layer in (0, 1):
                remote(out.at[layer], of("recv2").at[layer], "sent2", "recv2", second[layer])

        if stage == FETCH:
            for layer in (0, 1):
                local(w[i].at[at(layer, 0, 0)], of("w_in").at[layer], "recv2")
                local(m[i].at[layer, own], of("m_in").at[layer], "recv2")
                local(v[i].at[layer, own], of("v_in").at[layer], "recv2")

        if stage == STEP:
            near, came, last = of("near"), of("recv1"), of("recv2")
            w_in, m_in, v_in = of("w_in"), of("m_in"), of("v_in")
            take("recv2", 12)
            for layer in (0, 1):
                rows_of = at(layer, 0, 0)[1]

                def step(p, layer=layer, rows_of=rows_of):
                    gsum = near[(layer, 0, *p)].astype(F32) + other[(1, layer, 0, *p)].astype(F32)
                    gsum = gsum + came[(layer, 0, *p)].astype(F32) + last[(layer, *p)].astype(F32)
                    gsum = gsum.astype(BF16).astype(F32)
                    one = adamw(w_in[(layer, *p)].astype(F32), m_in[(layer, *p)], v_in[(layer, *p)], gsum)
                    if i == APART:
                        w_in[(layer, *p)] = one[0]
                    else:
                        new_w[i][layer, rows_of, p[1]] = one[0]
                    new_m[i][layer, own, p[1]] = one[1]
                    new_v[i][layer, own, p[1]] = one[2]
                pieces(step)
            take("sent2", 2)
            give(u, "partner", ((0, partner),))
            give(u, "recv1", ((1, near_x), (2, near_y)))
            for layer in (0, 1):
                if i == APART:
                    local(w_in.at[layer], new_w[i].at[layer, own], "ag1")
                    continue
                mine = new_w[i].at[at(layer, 0, 0)]
                remote(mine, mine, "sent3", "ag1", second[layer])
                remote(mine, mine, "sent3", "ag2", first[layer])
                remote(mine, mine, "sent3", "ag3", partner)

        if stage == AG1:
            take("ag1", 2)
            for layer in (0, 1) if i != APART else ():
                came = new_w[i].at[at(layer, 0, 1)]
                remote(came, came, "sent3", "ag2", first[layer])
            for layer in (0, 1) if i != APART else ():
                came = new_w[i].at[at(layer, 0, 1)]
                remote(came, came, "sent3", "ag3", partner)

        if stage == AG2 and i != APART:
            take("ag2", 4)
            for layer in (0, 1):
                for s in (0, 1):
                    came = new_w[i].at[at(layer, 1, s)]
                    remote(came, came, "sent3", "ag3", partner)

        if stage == END and i != APART:
            take("ag3", 8)
            take("sent3", 14)

    def body(t, _):
        for stage in ORDER:
            u = t - LAG[stage]
            for i, start, end, chunk, pos in spans:
                @pl.when(jnp.logical_and(u >= start, u < end))
                def _(i=i, start=start, chunk=chunk, pos=pos, stage=stage, u=u):
                    run(stage, i, u - start + chunk, u, u - start + pos)
        return 0

    lax.fori_loop(0, total + LAG[END], body, 0)


def finish(own, from_x, from_y, whole, hop, across, sent, sent_across):
    rows, cols = own.shape[1:]
    tall = CHUNK[cols]
    parts = rows // tall
    me = lax.axis_index("dp")
    x, y, core = me // 4, (me // 2) % 2, me % 2
    near_x, near_y, partner = me + 4 - 8 * x, me + 2 - 4 * y, me + 1 - 2 * core
    corner = (1 - x) * 4 + (1 - y) * 2 + core

    barrier = pltpu.get_barrier_semaphore()
    for other in (partner, near_x, near_y):
        pl.semaphore_signal(barrier, inc=1, device_id={"dp": other}, device_id_type=MESH)
    pl.semaphore_wait(barrier, 3)

    def place(layer, device, k, count):
        return whole.at[layer, pl.ds(pl.multiple_of(device * rows + k * tall, tall), count * tall)]

    def remote(src, dst, sent, received, other):
        pltpu.make_async_remote_copy(
            src_ref=src, dst_ref=dst, send_sem=sent, recv_sem=received, device_id={"dp": other}, device_id_type=MESH
        ).start()

    def take(sem, chunks):
        like = whole.at[0, pl.ds(0, chunks * tall)]
        pltpu.make_async_copy(like, like, sem).wait()

    for k in range(parts):
        for layer, came, device, other in ((0, from_y, near_y, near_x), (1, from_x, near_x, near_y)):
            remote(came.at[layer, pl.ds(k * tall, tall)], place(layer, device, k, 1), sent, hop.at[k], other)
    for layer in (0, 1):
        for src, device in ((own, me), (from_x, near_x), (from_y, near_y)):
            remote(src.at[layer], place(layer, device, 0, parts), sent_across, across, partner)
            pltpu.make_async_copy(src.at[layer], place(layer, device, 0, parts), hop.at[parts]).start()
    for k in range(parts):
        take(hop.at[k], 2)
        for layer in (0, 1):
            here = place(layer, corner, k, 1)
            remote(here, here, sent_across, across, partner)
    take(hop.at[parts], 6 * parts)
    take(across, 8 * parts)
    take(sent, 2 * parts)
    take(sent_across, 8 * parts)


def copy_out(n, *refs):
    copies = [
        pltpu.make_async_copy(src.at[layer], dst.at[layer], refs[2 * n])
        for src, dst in zip(refs[:n], refs[n : 2 * n], strict=True) for layer in (0, 1)
    ]
    for copy in copies:
        copy.start()
    for copy in copies:
        copy.wait()


def to_hbm(*arrays):
    n = len(arrays)
    return pl.pallas_call(
        functools.partial(copy_out, n),
        out_shape=tuple(jax.ShapeDtypeStruct(a.shape, a.dtype) for a in arrays),
        in_specs=[pl.BlockSpec(memory_space=pl.ANY)] * n,
        out_specs=(pl.BlockSpec(memory_space=pl.ANY),) * n,
        scratch_shapes=[pltpu.SemaphoreType.DMA],
        cost_estimate=pl.CostEstimate(flops=10**8, bytes_accessed=2 * 10**7, transcendentals=0),
        compiler_params=pltpu.CompilerParams(vmem_limit_bytes=2**20),
    )(*arrays)


def solution(mesh):
    def step(*arrays):
        terms, weights, m, v = (arrays[i : i + 3] for i in (0, 3, 6, 9))
        widths = sorted({one.shape[2] for one in m})
        scratch = [pltpu.VMEM((slots, *held, CHUNK[cols], cols), kind) for cols in widths for slots, held, kind in BUFFERS.values()]
        sems = [pltpu.SemaphoreType.DMA((slots,)) for slots in SEMS.values()]
        part = jax.ShapeDtypeStruct(m[APART].shape, BF16)
        out = pl.pallas_call(
            kernel,
            out_shape=tuple(pltpu.VMEM(one.shape, one.dtype) if k != APART else part for k, one in enumerate((*weights, *m, *v))),
            in_specs=[pl.BlockSpec(memory_space=pl.ANY)] * 12,
            out_specs=tuple(pl.BlockSpec(memory_space=pltpu.VMEM if k != APART else pltpu.HBM) for k in range(9)),
            scratch_shapes=[*scratch, *sems, pltpu.SemaphoreType.REGULAR((3,))],
            compiler_params=pltpu.CompilerParams(collective_id=0, has_side_effects=True, vmem_limit_bytes=23 * 2**20),
        )(*(t[0] for t in terms), *weights, *m, *v)
        own = out[APART]
        from_x, from_y = (lax.ppermute(own, "dp", [(d, d ^ flip) for d in range(8)]) for flip in (4, 2))
        parts = part.shape[1] // CHUNK[part.shape[2]]
        gate, *moments = to_hbm(out[0], *out[3:])
        down = to_hbm(out[2])[0]
        whole = pl.pallas_call(
            finish,
            out_shape=pltpu.VMEM(weights[APART].shape, BF16),
            in_specs=[pl.BlockSpec(memory_space=pltpu.HBM)] * 3,
            out_specs=pl.BlockSpec(memory_space=pltpu.VMEM),
            scratch_shapes=[pltpu.SemaphoreType.DMA((parts + 1,))] + [pltpu.SemaphoreType.DMA] * 3,
            compiler_params=pltpu.CompilerParams(collective_id=1, has_side_effects=True, vmem_limit_bytes=2**20),
        )(own, from_x, from_y)
        return (gate, to_hbm(whole)[0], down, *moments)

    all_of, cut = P(None, None, None), P(None, "dp", None)
    return jax.shard_map(
        step,
        mesh=mesh,
        in_specs=(P(("rep", "dp"), None, None, None),) * 3 + (all_of,) * 3 + (cut,) * 6,
        out_specs=(P("rep", None, None),) * 3 + (P("rep", "dp", None),) * 6,
        check_vma=False,
    )
```

```python
import functools

import jax
import jax.numpy as jnp
from jax import lax
from jax.experimental import pallas as pl
from jax.experimental.pallas import tpu as pltpu
from jax.sharding import PartitionSpec as P

MESH = pl.DeviceIdType.MESH
F32, BF16 = jnp.float32, jnp.bfloat16

LOAD, RS1, RS2, FETCH, STEP, AG1, AG2, END = range(8)
LAG = (0, 1, 3, 4, 5, 7, 9, 10)
ORDER = (END, LOAD, RS1, RS2, FETCH, STEP, AG1, AG2)
RUNS = ((2, 0, 1, 1), (1, 3, 7, 7), (1, 0, 3, 7), (0, 0, 1, 1))
APART, SOONER = 1, 3
CHUNK = {2560: 16, 896: 32}
AHEAD = {"partner": 7, "recv1": 6, "recv2": 6}
WIDE = 512

BUFFERS = {
    "far": (2, (2, 2), BF16),
    "near": (6, (2, 2), BF16),
    "partner": (AHEAD["partner"], (2, 2, 2), BF16),
    "send1": (3, (2, 2), BF16),
    "recv1": (AHEAD["recv1"], (2, 2), BF16),
    "send2": (3, (2,), BF16),
    "recv2": (AHEAD["recv2"], (2,), BF16),
    "w_in": (4, (2,), BF16),
    "m_in": (2, (2,), F32),
    "v_in": (2, (2,), F32),
}
SEMS = {"far": 7, "near": 7, "sent1": 4, "recv1": 6, "recv2": 6, "sent2": 3, "ag1": 5, "ag2": 9, "ag3": 10, "sent3": 5}


def adamw(w, m, v, g):
    m = 0.9 * m + 0.1 * g
    v = 0.95 * v + 0.05 * g * g
    step = m * lax.rsqrt(v + 1e-8) + 0.1 * w
    return (w - 0.02 * step).astype(BF16), m, v


def kernel(*refs):
    g, w, m, v = (refs[i : i + 3] for i in (0, 3, 6, 9))
    new_w, new_m, new_v = (refs[i : i + 3] for i in (12, 15, 18))
    own_apart = refs[21]
    refs = list(refs[22:])
    widths = sorted({one.shape[2] for one in m})
    buf = {cols: {name: refs.pop(0) for name in BUFFERS} for cols in widths}
    sem = {name: refs.pop(0) for name in SEMS}
    credit = refs.pop(0)

    spans, total, done = [], 0, dict.fromkeys(widths, 0)
    for i, start, end, parts in RUNS:
        rows, cols = m[i].shape[1:]
        n = rows // CHUNK[cols]
        a, b = n * start // parts, n * end // parts
        spans.append((i, total, total + b - a, a, done[cols]))
        total += b - a
        done[cols] += b - a

    me = lax.axis_index("dp")
    x, y, core = me // 4, (me // 2) % 2, me % 2
    near_x, near_y, partner = me + 4 - 8 * x, me + 2 - 4 * y, me + 1 - 2 * core
    first, second = (near_x, near_y), (near_y, near_x)

    barrier = pltpu.get_barrier_semaphore()
    for other in (partner, near_x, near_y):
        pl.semaphore_signal(barrier, inc=1, device_id={"dp": other}, device_id_type=MESH)
    pl.semaphore_wait(barrier, 3)

    def block(layer, f, s, c):
        fx, fy = (f, s) if layer == 0 else (s, f)
        return (x + fx - 2 * x * fx) * 4 + (y + fy - 2 * y * fy) * 2 + c

    def give(u, name, others):
        @pl.when(u + AHEAD[name] < total)
        def _():
            for k, other in others:
                pl.semaphore_signal(credit.at[k], inc=1, device_id={"dp": other}, device_id_type=MESH)

    def spend(u, name, ks):
        @pl.when(u >= AHEAD[name])
        def _():
            for k in ks:
                pl.semaphore_wait(credit.at[k], 1)

    def run(stage, i, j, u, pos, apart):
        rows, cols = m[i].shape[1:]
        b = buf[cols]
        wide = WIDE if cols % WIDE == 0 else cols
        tall = CHUNK[cols]

        def at(layer, f, s, c=core):
            return (layer, pl.ds(pl.multiple_of(block(layer, f, s, c) * rows + j * tall, tall), tall))

        def of(name):
            return b[name].at[lax.rem(pos, b[name].shape[0])]

        def signal(name):
            return sem[name].at[lax.rem(u, sem[name].shape[0])]

        def take(name, chunks):
            like = g[i].at[0, pl.ds(0, chunks * tall)]
            pltpu.make_async_copy(like, like, signal(name)).wait()

        def local(src, dst, name):
            pltpu.make_async_copy(src, dst, signal(name)).start()

        def remote(src, dst, sent, received, other):
            pltpu.make_async_remote_copy(
                src_ref=src, dst_ref=dst, send_sem=signal(sent), recv_sem=signal(received),
                device_id={"dp": other}, device_id_type=MESH,
            ).start()

        def pieces(body):
            def one(k, _):
                body((slice(None), pl.ds(pl.multiple_of(k * wide, 128), wide)))
                return 0

            lax.fori_loop(0, cols // wide, one, 0)

        own = pl.ds(pl.multiple_of(j * tall, tall), tall)
        other = of("partner")

        if stage == LOAD:
            spend(u, "partner", (0,))
            for side, mine in ((1, "far"), (0, "near")):
                for layer in (0, 1):
                    for s in (0, 1):
                        remote(g[i].at[at(layer, side, s, 1 - core)], other.at[1 - side, layer, s], "sent1", mine, partner)
                for layer in (0, 1):
                    for s in (0, 1):
                        local(g[i].at[at(layer, side, s)], of(mine).at[layer, s], mine)

        if stage == RS1:
            far, out = of("far"), of("send1")
            take("far", 8)
            for layer in (0, 1):
                for s in (0, 1):
                    def add(p, layer=layer, s=s):
                        out[(layer, s, *p)] = (far[(layer, s, *p)].astype(F32) + other[(0, layer, s, *p)].astype(F32)).astype(BF16)
                    pieces(add)
            spend(u, "recv1", (1, 2))
            for layer in (0, 1):
                remote(out.at[layer], of("recv1").at[layer], "sent1", "recv1", first[layer])

        if stage == RS2:
            near, came, out = of("near"), of("recv1"), of("send2")
            take("near", 8)
            take("recv1", 4)
            for layer in (0, 1):
                def add(p, layer=layer):
                    out[(layer, *p)] = (
                        near[(layer, 1, *p)].astype(F32) + other[(1, layer, 1, *p)].astype(F32) + came[(layer, 1, *p)].astype(F32)
                    ).astype(BF16)
                pieces(add)
            take("sent1", 12)
            for layer in (0, 1):
                remote(out.at[layer], of("recv2").at[layer], "sent2", "recv2", second[layer])

        if stage == FETCH:
            for layer in (0, 1):
                local(w[i].at[at(layer, 0, 0)], of("w_in").at[layer], "recv2")
                local(m[i].at[layer, own], of("m_in").at[layer], "recv2")
                local(v[i].at[layer, own], of("v_in").at[layer], "recv2")

        if stage == STEP:
            near, came, last = of("near"), of("recv1"), of("recv2")
            w_in, m_in, v_in = of("w_in"), of("m_in"), of("v_in")
            take("recv2", 12)
            for layer in (0, 1):
                rows_of = at(layer, 0, 0)[1]

                def step(p, layer=layer, rows_of=rows_of):
                    gsum = near[(layer, 0, *p)].astype(F32) + other[(1, layer, 0, *p)].astype(F32)
                    gsum = gsum + came[(layer, 0, *p)].astype(F32) + last[(layer, *p)].astype(F32)
                    gsum = gsum.astype(BF16).astype(F32)
                    one = adamw(w_in[(layer, *p)].astype(F32), m_in[(layer, *p)], v_in[(layer, *p)], gsum)
                    if apart:
                        w_in[(layer, *p)] = one[0]
                    else:
                        new_w[i][layer, rows_of, p[1]] = one[0]
                    new_m[i][layer, own, p[1]] = one[1]
                    new_v[i][layer, own, p[1]] = one[2]
                pieces(step)
            take("sent2", 2)
            give(u, "partner", ((0, partner),))
            give(u, "recv1", ((1, near_x), (2, near_y)))
            for layer in (0, 1):
                if apart:
                    there = pl.ds(pl.multiple_of((j - SOONER) * tall, tall), tall)
                    local(w_in.at[layer], own_apart.at[layer, there], "ag1")
                    continue
                mine = new_w[i].at[at(layer, 0, 0)]
                remote(mine, mine, "sent3", "ag1", second[layer])
                remote(mine, mine, "sent3", "ag2", first[layer])
                remote(mine, mine, "sent3", "ag3", partner)

        if stage == AG1:
            take("ag1", 2)
            for layer in (0, 1) if not apart else ():
                came = new_w[i].at[at(layer, 0, 1)]
                remote(came, came, "sent3", "ag2", first[layer])
            for layer in (0, 1) if not apart else ():
                came = new_w[i].at[at(layer, 0, 1)]
                remote(came, came, "sent3", "ag3", partner)

        if stage == AG2 and not apart:
            take("ag2", 4)
            for layer in (0, 1):
                for s in (0, 1):
                    came = new_w[i].at[at(layer, 1, s)]
                    remote(came, came, "sent3", "ag3", partner)

        if stage == END and not apart:
            take("ag3", 8)
            take("sent3", 14)

    def body(t, _):
        for stage in ORDER:
            u = t - LAG[stage]
            for i, start, end, chunk, pos in spans:
                @pl.when(jnp.logical_and(u >= start, u < end))
                def _(i=i, start=start, chunk=chunk, pos=pos, stage=stage, u=u):
                    run(stage, i, u - start + chunk, u, u - start + pos, i == APART and chunk >= SOONER)
        return 0

    lax.fori_loop(0, total + LAG[END], body, 0)


def finish(own, from_x, from_y, whole, hop, across, sent, sent_across):
    rows, cols = own.shape[1:]
    tall = CHUNK[cols]
    parts = rows // tall
    me = lax.axis_index("dp")
    x, y, core = me // 4, (me // 2) % 2, me % 2
    near_x, near_y, partner = me + 4 - 8 * x, me + 2 - 4 * y, me + 1 - 2 * core
    corner = (1 - x) * 4 + (1 - y) * 2 + core

    barrier = pltpu.get_barrier_semaphore()
    for other in (partner, near_x, near_y):
        pl.semaphore_signal(barrier, inc=1, device_id={"dp": other}, device_id_type=MESH)
    pl.semaphore_wait(barrier, 3)

    def place(layer, device, k, count):
        return whole.at[layer, pl.ds(pl.multiple_of(device * rows + k * tall, tall), count * tall)]

    def remote(src, dst, sent, received, other):
        pltpu.make_async_remote_copy(
            src_ref=src, dst_ref=dst, send_sem=sent, recv_sem=received, device_id={"dp": other}, device_id_type=MESH
        ).start()

    def take(sem, chunks):
        like = whole.at[0, pl.ds(0, chunks * tall)]
        pltpu.make_async_copy(like, like, sem).wait()

    for k in range(parts):
        for layer, came, device, other in ((0, from_y, near_y, near_x), (1, from_x, near_x, near_y)):
            remote(came.at[layer, pl.ds(k * tall, tall)], place(layer, device, k, 1), sent, hop.at[k], other)
    for layer in (0, 1):
        for src, device in ((own, me), (from_x, near_x), (from_y, near_y)):
            remote(src.at[layer], place(layer, device, 0, parts), sent_across, across, partner)
            pltpu.make_async_copy(src.at[layer], place(layer, device, 0, parts), hop.at[parts]).start()
    for k in range(parts):
        take(hop.at[k], 2)
        for layer in (0, 1):
            here = place(layer, corner, k, 1)
            remote(here, here, sent_across, across, partner)
    take(hop.at[parts], 6 * parts)
    take(across, 8 * parts)
    take(sent, 2 * parts)
    take(sent_across, 8 * parts)


def run_copies(copies):
    for copy in copies:
        copy.start()
    for copy in copies:
        copy.wait()


def copy_whole(n, *refs):
    run_copies([
        pltpu.make_async_copy(src.at[layer], dst.at[layer], refs[2 * n])
        for src, dst in zip(refs[:n], refs[n : 2 * n], strict=True) for layer in (0, 1)
    ])


def copy_sooner(down, up, new_down, new_up, sem):
    run_copies(
        [pltpu.make_async_copy(down.at[layer], new_down.at[layer], sem) for layer in (0, 1)]
        + [pltpu.make_async_copy(up.at[at], new_up.at[at], sem) for at in sooner_and_later(up.shape[1] // 8)[0]]
    )


def copy_later(_, piece, new_up, sem):
    _, later = sooner_and_later(new_up.shape[1] // 8)
    run_copies([pltpu.make_async_copy(piece.at[src], new_up.at[dst], sem) for src, dst in later])


def sooner_and_later(rows):
    first = SOONER * CHUNK[2560]
    rest = rows - first
    each = [(layer, block) for layer in (0, 1) for block in range(8)]
    return (
        [(layer, pl.ds(block * rows, first)) for layer, block in each],
        [((layer, pl.ds(block * rest, rest)), (layer, pl.ds(block * rows + first, rest))) for layer, block in each],
    )


def plain(body, arrays, like, **more):
    return pl.pallas_call(
        body,
        out_shape=tuple(jax.ShapeDtypeStruct(a.shape, a.dtype) for a in like),
        in_specs=[pl.BlockSpec(memory_space=pl.ANY)] * len(arrays),
        out_specs=(pl.BlockSpec(memory_space=pl.ANY),) * len(like),
        scratch_shapes=[pltpu.SemaphoreType.DMA],
        cost_estimate=pl.CostEstimate(flops=10**8, bytes_accessed=2 * 10**7, transcendentals=0),
        compiler_params=pltpu.CompilerParams(vmem_limit_bytes=2**20),
        **more,
    )(*arrays)


def solution(mesh):
    def step(*arrays):
        terms, weights, m, v = (arrays[i : i + 3] for i in (0, 3, 6, 9))
        widths = sorted({one.shape[2] for one in m})
        scratch = [pltpu.VMEM((slots, *held, CHUNK[cols], cols), kind) for cols in widths for slots, held, kind in BUFFERS.values()]
        sems = [pltpu.SemaphoreType.DMA((slots,)) for slots in SEMS.values()]
        rows, cols = m[APART].shape[1:]
        left = rows - SOONER * CHUNK[cols]
        out = pl.pallas_call(
            kernel,
            out_shape=(*(pltpu.VMEM(one.shape, one.dtype) for one in (*weights, *m, *v)), jax.ShapeDtypeStruct((2, left, cols), BF16)),
            in_specs=[pl.BlockSpec(memory_space=pl.ANY)] * 12,
            out_specs=(pl.BlockSpec(memory_space=pltpu.VMEM),) * 9 + (pl.BlockSpec(memory_space=pltpu.HBM),),
            scratch_shapes=[*scratch, *sems, pltpu.SemaphoreType.REGULAR((3,))],
            compiler_params=pltpu.CompilerParams(collective_id=0, has_side_effects=True, vmem_limit_bytes=int(23 * 2**20)),
        )(*(t[0] for t in terms), *weights, *m, *v)
        gate, up, down, *moments, own = out
        from_x, from_y = (lax.ppermute(own, "dp", [(d, d ^ flip) for d in range(8)]) for flip in (4, 2))
        gate, *moments = plain(functools.partial(copy_whole, 7), (gate, *moments), (gate, *moments))
        down, up = plain(copy_sooner, (down, up), (down, up))
        piece = pl.pallas_call(
            finish,
            out_shape=pltpu.VMEM((2, 8 * left, cols), BF16),
            in_specs=[pl.BlockSpec(memory_space=pltpu.HBM)] * 3,
            out_specs=pl.BlockSpec(memory_space=pltpu.VMEM),
            scratch_shapes=[pltpu.SemaphoreType.DMA((left // CHUNK[cols] + 1,))] + [pltpu.SemaphoreType.DMA] * 3,
            compiler_params=pltpu.CompilerParams(collective_id=1, has_side_effects=True, vmem_limit_bytes=2**20),
        )(own, from_x, from_y)
        (up,) = plain(copy_later, (up, piece), (up,), input_output_aliases={0: 0})
        return (gate, up, down, *moments)

    all_of, cut = P(None, None, None), P(None, "dp", None)
    return jax.shard_map(
        step,
        mesh=mesh,
        in_specs=(P(("rep", "dp"), None, None, None),) * 3 + (all_of,) * 3 + (cut,) * 6,
        out_specs=(P("rep", None, None),) * 3 + (P("rep", "dp", None),) * 6,
        check_vma=False,
    )
```

```python
import functools

import jax
import jax.numpy as jnp
from jax import lax
from jax.experimental import pallas as pl
from jax.experimental.pallas import tpu as pltpu
from jax.sharding import PartitionSpec as P

MESH = pl.DeviceIdType.MESH
F32, BF16 = jnp.float32, jnp.bfloat16

LOAD, RS1, RS2, FETCH, STEP, AG1, AG2, END = range(8)
LAG = (0, 1, 3, 4, 5, 7, 9, 10)
ORDER = (END, LOAD, RS1, RS2, FETCH, STEP, AG1, AG2)
RUNS = ((2, 0, 1, 1), (1, 3, 7, 7), (0, 0, 1, 1), (1, 0, 3, 7))
APART, SOONER = 1, 3
CHUNK = {2560: 16, 896: 32}
AHEAD = {"partner": 7, "recv1": 6, "recv2": 6}
WIDE = 512

BUFFERS = {
    "far": (2, (2, 2), BF16),
    "near": (6, (2, 2), BF16),
    "partner": (AHEAD["partner"], (2, 2, 2), BF16),
    "send1": (3, (2, 2), BF16),
    "recv1": (AHEAD["recv1"], (2, 2), BF16),
    "send2": (3, (2,), BF16),
    "recv2": (AHEAD["recv2"], (2,), BF16),
    "w_in": (2, (2,), BF16),
    "m_in": (2, (2,), F32),
    "v_in": (2, (2,), F32),
}
SEMS = {"far": 7, "near": 7, "sent1": 4, "recv1": 6, "recv2": 6, "sent2": 3, "ag1": 5, "ag2": 9, "ag3": 10, "sent3": 5}


def adamw(w, m, v, g):
    m = 0.9 * m + 0.1 * g
    v = 0.95 * v + 0.05 * g * g
    step = m * lax.rsqrt(v + 1e-8) + 0.1 * w
    return (w - 0.02 * step).astype(BF16), m, v


def kernel(*refs):
    g, w, m, v = (refs[i : i + 3] for i in (0, 3, 6, 9))
    new_w, new_m, new_v = (refs[i : i + 3] for i in (12, 15, 18))
    own_apart = refs[21]
    refs = list(refs[22:])
    widths = sorted({one.shape[2] for one in m})
    buf = {cols: {name: refs.pop(0) for name in BUFFERS} for cols in widths}
    sem = {name: refs.pop(0) for name in SEMS}
    credit = refs.pop(0)

    spans, total, done = [], 0, dict.fromkeys(widths, 0)
    for i, start, end, parts in RUNS:
        rows, cols = m[i].shape[1:]
        n = rows // CHUNK[cols]
        a, b = n * start // parts, n * end // parts
        spans.append((i, total, total + b - a, a, done[cols]))
        total += b - a
        done[cols] += b - a

    me = lax.axis_index("dp")
    x, y, core = me // 4, (me // 2) % 2, me % 2
    near_x, near_y, partner = me + 4 - 8 * x, me + 2 - 4 * y, me + 1 - 2 * core
    first, second = (near_x, near_y), (near_y, near_x)

    barrier = pltpu.get_barrier_semaphore()
    for other in (partner, near_x, near_y):
        pl.semaphore_signal(barrier, inc=1, device_id={"dp": other}, device_id_type=MESH)
    pl.semaphore_wait(barrier, 3)

    def block(layer, f, s, c):
        fx, fy = (f, s) if layer == 0 else (s, f)
        return (x + fx - 2 * x * fx) * 4 + (y + fy - 2 * y * fy) * 2 + c

    def give(u, name, others):
        @pl.when(u + AHEAD[name] < total)
        def _():
            for k, other in others:
                pl.semaphore_signal(credit.at[k], inc=1, device_id={"dp": other}, device_id_type=MESH)

    def spend(u, name, ks):
        @pl.when(u >= AHEAD[name])
        def _():
            for k in ks:
                pl.semaphore_wait(credit.at[k], 1)

    def run(stage, i, j, u, pos, apart):
        rows, cols = m[i].shape[1:]
        b = buf[cols]
        wide = WIDE if cols % WIDE == 0 else cols
        tall = CHUNK[cols]

        def at(layer, f, s, c=core):
            return (layer, pl.ds(pl.multiple_of(block(layer, f, s, c) * rows + j * tall, tall), tall))

        def of(name):
            return b[name].at[lax.rem(pos, b[name].shape[0])]

        def signal(name):
            return sem[name].at[lax.rem(u, sem[name].shape[0])]

        def take(name, chunks):
            like = g[i].at[0, pl.ds(0, chunks * tall)]
            pltpu.make_async_copy(like, like, signal(name)).wait()

        def local(src, dst, name):
            pltpu.make_async_copy(src, dst, signal(name)).start()

        def remote(src, dst, sent, received, other):
            pltpu.make_async_remote_copy(
                src_ref=src, dst_ref=dst, send_sem=signal(sent), recv_sem=signal(received),
                device_id={"dp": other}, device_id_type=MESH,
            ).start()

        def pieces(body):
            def one(k, _):
                body((slice(None), pl.ds(pl.multiple_of(k * wide, 128), wide)))
                return 0

            lax.fori_loop(0, cols // wide, one, 0)

        own = pl.ds(pl.multiple_of(j * tall, tall), tall)
        other = of("partner")

        if stage == LOAD:
            spend(u, "partner", (0,))
            for side, mine in ((1, "far"), (0, "near")):
                for layer in (0, 1):
                    for s in (0, 1):
                        remote(g[i].at[at(layer, side, s, 1 - core)], other.at[1 - side, layer, s], "sent1", mine, partner)
                for layer in (0, 1):
                    for s in (0, 1):
                        local(g[i].at[at(layer, side, s)], of(mine).at[layer, s], mine)

        if stage == RS1:
            far, out = of("far"), of("send1")
            take("far", 8)
            for layer in (0, 1):
                for s in (0, 1):
                    def add(p, layer=layer, s=s):
                        out[(layer, s, *p)] = (far[(layer, s, *p)].astype(F32) + other[(0, layer, s, *p)].astype(F32)).astype(BF16)
                    pieces(add)
            spend(u, "recv1", (1, 2))
            for layer in (0, 1):
                remote(out.at[layer], of("recv1").at[layer], "sent1", "recv1", first[layer])

        if stage == RS2:
            near, came, out = of("near"), of("recv1"), of("send2")
            take("near", 8)
            take("recv1", 4)
            for layer in (0, 1):
                def add(p, layer=layer):
                    out[(layer, *p)] = (
                        near[(layer, 1, *p)].astype(F32) + other[(1, layer, 1, *p)].astype(F32) + came[(layer, 1, *p)].astype(F32)
                    ).astype(BF16)
                pieces(add)
            take("sent1", 12)
            for layer in (0, 1):
                remote(out.at[layer], of("recv2").at[layer], "sent2", "recv2", second[layer])

        if stage == FETCH:
            for layer in (0, 1):
                local(w[i].at[at(layer, 0, 0)], of("w_in").at[layer], "recv2")
                local(m[i].at[layer, own], of("m_in").at[layer], "recv2")
                local(v[i].at[layer, own], of("v_in").at[layer], "recv2")

        if stage == STEP:
            near, came, last = of("near"), of("recv1"), of("recv2")
            w_in, m_in, v_in = of("w_in"), of("m_in"), of("v_in")
            take("recv2", 12)
            for layer in (0, 1):
                rows_of = at(layer, 0, 0)[1]

                def step(p, layer=layer, rows_of=rows_of):
                    gsum = near[(layer, 0, *p)].astype(F32) + other[(1, layer, 0, *p)].astype(F32)
                    gsum = gsum + came[(layer, 0, *p)].astype(F32) + last[(layer, *p)].astype(F32)
                    gsum = gsum.astype(BF16).astype(F32)
                    one = adamw(w_in[(layer, *p)].astype(F32), m_in[(layer, *p)], v_in[(layer, *p)], gsum)
                    if apart:
                        own_apart[layer, pl.ds(pl.multiple_of((j - SOONER) * tall, tall), tall), p[1]] = one[0]
                    else:
                        new_w[i][layer, rows_of, p[1]] = one[0]
                    new_m[i][layer, own, p[1]] = one[1]
                    new_v[i][layer, own, p[1]] = one[2]
                pieces(step)
            take("sent2", 2)
            give(u, "partner", ((0, partner),))
            give(u, "recv1", ((1, near_x), (2, near_y)))
            for layer in (0, 1):
                if apart:
                    continue
                mine = new_w[i].at[at(layer, 0, 0)]
                remote(mine, mine, "sent3", "ag1", second[layer])
                remote(mine, mine, "sent3", "ag2", first[layer])
                remote(mine, mine, "sent3", "ag3", partner)

        if stage == AG1 and not apart:
            take("ag1", 2)
            for layer in (0, 1):
                came = new_w[i].at[at(layer, 0, 1)]
                remote(came, came, "sent3", "ag2", first[layer])
            for layer in (0, 1):
                came = new_w[i].at[at(layer, 0, 1)]
                remote(came, came, "sent3", "ag3", partner)

        if stage == AG2 and not apart:
            take("ag2", 4)

            @pl.when(u < total - 1)
            def _():
                for layer in (0, 1):
                    for s in (0, 1):
                        came = new_w[i].at[at(layer, 1, s)]
                        remote(came, came, "sent3", "ag3", partner)

        if stage == END and not apart:
            @pl.when(u < total - 1)
            def _():
                take("ag3", 8)
                take("sent3", 14)

            @pl.when(u == total - 1)
            def _():
                take("ag3", 4)
                take("sent3", 10)

    def body(t, _):
        for stage in ORDER:
            u = t - LAG[stage]
            for i, start, end, chunk, pos in spans:
                @pl.when(jnp.logical_and(u >= start, u < end))
                def _(i=i, start=start, chunk=chunk, pos=pos, stage=stage, u=u):
                    run(stage, i, u - start + chunk, u, u - start + pos, i == APART and chunk >= SOONER)
        return 0

    lax.fori_loop(0, total + LAG[END], body, 0)


def far_last(up, layer, s, x, y, core):
    fx, fy = ((1 - x), (1 - y if s else y)) if layer == 0 else ((1 - x if s else x), (1 - y))
    tall, rows = CHUNK[up.shape[2]], up.shape[1] // 8
    start = (fx * 4 + fy * 2 + core) * rows + (SOONER - 1) * tall
    return up.at[layer, pl.ds(pl.multiple_of(start, tall), tall)]


def finish(own, from_x, from_y, up, whole, extra, hop, across, sent, sent_across, across_extra, sent_extra):
    rows, cols = own.shape[1:]
    tall = CHUNK[cols]
    parts = rows // tall
    me = lax.axis_index("dp")
    x, y, core = me // 4, (me // 2) % 2, me % 2
    near_x, near_y, partner = me + 4 - 8 * x, me + 2 - 4 * y, me + 1 - 2 * core
    corner = (1 - x) * 4 + (1 - y) * 2 + core

    barrier = pltpu.get_barrier_semaphore()
    for other in (partner, near_x, near_y):
        pl.semaphore_signal(barrier, inc=1, device_id={"dp": other}, device_id_type=MESH)
    pl.semaphore_wait(barrier, 3)

    def place(layer, device, k, count):
        return whole.at[layer, pl.ds(pl.multiple_of(device * rows + k * tall, tall), count * tall)]

    def remote(src, dst, sent, received, other):
        pltpu.make_async_remote_copy(
            src_ref=src, dst_ref=dst, send_sem=sent, recv_sem=received, device_id={"dp": other}, device_id_type=MESH
        ).start()

    def take(sem, chunks):
        like = whole.at[0, pl.ds(0, chunks * tall)]
        pltpu.make_async_copy(like, like, sem).wait()

    for k in range(parts):
        for layer, came, device, other in ((0, from_y, near_y, near_x), (1, from_x, near_x, near_y)):
            remote(came.at[layer, pl.ds(k * tall, tall)], place(layer, device, k, 1), sent, hop.at[k], other)
    for layer in (0, 1):
        for s in (0, 1):
            remote(far_last(up, layer, s, x, y, core), extra.at[layer, s], sent_extra, across_extra, partner)
    for layer in (0, 1):
        for src, device in ((own, me), (from_x, near_x), (from_y, near_y)):
            remote(src.at[layer], place(layer, device, 0, parts), sent_across, across, partner)
            pltpu.make_async_copy(src.at[layer], place(layer, device, 0, parts), hop.at[parts]).start()
    for k in range(parts):
        take(hop.at[k], 2)
        for layer in (0, 1):
            here = place(layer, corner, k, 1)
            remote(here, here, sent_across, across, partner)
    take(hop.at[parts], 6 * parts)
    take(across, 8 * parts)
    take(sent, 2 * parts)
    take(sent_across, 8 * parts)
    take(across_extra, 4)
    take(sent_extra, 4)


def run_copies(copies):
    for copy in copies:
        copy.start()
    for copy in copies:
        copy.wait()


def copy_whole(n, *refs):
    run_copies([
        pltpu.make_async_copy(src.at[layer], dst.at[layer], refs[2 * n])
        for src, dst in zip(refs[:n], refs[n : 2 * n], strict=True) for layer in (0, 1)
    ])


def copy_sooner(down, up, new_down, new_up, sem):
    run_copies(
        [pltpu.make_async_copy(down.at[layer], new_down.at[layer], sem) for layer in (0, 1)]
        + [pltpu.make_async_copy(up.at[at], new_up.at[at], sem) for at in sooner_and_later(up.shape[1] // 8)[0]]
    )


def copy_later(_, piece, extra, new_up, sem):
    _, later = sooner_and_later(new_up.shape[1] // 8)
    me = lax.axis_index("dp")
    x, y, core = me // 4, (me // 2) % 2, me % 2
    run_copies(
        [pltpu.make_async_copy(piece.at[src], new_up.at[dst], sem) for src, dst in later]
        + [pltpu.make_async_copy(extra.at[layer, s], far_last(new_up, layer, s, x, y, 1 - core), sem) for layer in (0, 1) for s in (0, 1)]
    )


def sooner_and_later(rows):
    first = SOONER * CHUNK[2560]
    rest = rows - first
    each = [(layer, block) for layer in (0, 1) for block in range(8)]
    return (
        [(layer, pl.ds(block * rows, first)) for layer, block in each],
        [((layer, pl.ds(block * rest, rest)), (layer, pl.ds(block * rows + first, rest))) for layer, block in each],
    )


def plain(body, arrays, like, **more):
    return pl.pallas_call(
        body,
        out_shape=tuple(jax.ShapeDtypeStruct(a.shape, a.dtype) for a in like),
        in_specs=[pl.BlockSpec(memory_space=pl.ANY)] * len(arrays),
        out_specs=(pl.BlockSpec(memory_space=pl.ANY),) * len(like),
        scratch_shapes=[pltpu.SemaphoreType.DMA],
        cost_estimate=pl.CostEstimate(flops=10**8, bytes_accessed=2 * 10**7, transcendentals=0),
        compiler_params=pltpu.CompilerParams(vmem_limit_bytes=2**20),
        **more,
    )(*arrays)


def solution(mesh):
    def step(*arrays):
        terms, weights, m, v = (arrays[i : i + 3] for i in (0, 3, 6, 9))
        widths = sorted({one.shape[2] for one in m})
        scratch = [pltpu.VMEM((slots, *held, CHUNK[cols], cols), kind) for cols in widths for slots, held, kind in BUFFERS.values()]
        sems = [pltpu.SemaphoreType.DMA((slots,)) for slots in SEMS.values()]
        rows, cols = m[APART].shape[1:]
        left = rows - SOONER * CHUNK[cols]
        out = pl.pallas_call(
            kernel,
            out_shape=(*(pltpu.VMEM(one.shape, one.dtype) for one in (*weights, *m, *v)), pltpu.VMEM((2, left, cols), BF16)),
            in_specs=[pl.BlockSpec(memory_space=pl.ANY)] * 12,
            out_specs=(pl.BlockSpec(memory_space=pltpu.VMEM),) * 10,
            scratch_shapes=[*scratch, *sems, pltpu.SemaphoreType.REGULAR((3,))],
            compiler_params=pltpu.CompilerParams(collective_id=0, has_side_effects=True, vmem_limit_bytes=int(23 * 2**20)),
        )(*(t[0] for t in terms), *weights, *m, *v)
        gate, up, down, *moments, own = out
        from_x, from_y = (lax.ppermute(own, "dp", [(d, d ^ flip) for d in range(8)]) for flip in (4, 2))
        gate, *moments = plain(functools.partial(copy_whole, 7), (gate, *moments), (gate, *moments))
        down, new_up = plain(copy_sooner, (down, up), (down, up))
        piece, extra = pl.pallas_call(
            finish,
            out_shape=(pltpu.VMEM((2, 8 * left, cols), BF16), pltpu.VMEM((2, 2, CHUNK[cols], cols), BF16)),
            in_specs=[pl.BlockSpec(memory_space=pl.ANY)] * 4,
            out_specs=(pl.BlockSpec(memory_space=pltpu.VMEM),) * 2,
            scratch_shapes=[pltpu.SemaphoreType.DMA((left // CHUNK[cols] + 1,))] + [pltpu.SemaphoreType.DMA] * 5,
            compiler_params=pltpu.CompilerParams(collective_id=1, has_side_effects=True, vmem_limit_bytes=2**20),
        )(own, from_x, from_y, up)
        (up,) = plain(copy_later, (new_up, piece, extra), (new_up,), input_output_aliases={0: 0})
        return (gate, up, down, *moments)

    all_of, cut = P(None, None, None), P(None, "dp", None)
    return jax.shard_map(
        step,
        mesh=mesh,
        in_specs=(P(("rep", "dp"), None, None, None),) * 3 + (all_of,) * 3 + (cut,) * 6,
        out_specs=(P("rep", None, None),) * 3 + (P("rep", "dp", None),) * 6,
        check_vma=False,
    )
```

```python
import functools

import jax
import jax.numpy as jnp
from jax import lax
from jax.experimental import pallas as pl
from jax.experimental.pallas import tpu as pltpu
from jax.sharding import PartitionSpec as P

MESH = pl.DeviceIdType.MESH
F32, BF16 = jnp.float32, jnp.bfloat16

LOAD, RS1, RS2, FETCH, STEP, AG1, AG2, END = range(8)
LAG = (0, 1, 2, 3, 4, 5, 6, 7)
ORDER = (END, LOAD, RS1, RS2, FETCH, STEP, AG1, AG2)
RUNS = ((2, 0, 1, 1), (1, 3, 7, 7), (0, 0, 1, 1), (1, 0, 3, 7))
APART, SOONER = 1, 3
CHUNK = {2560: 16, 896: 32}
AHEAD = {"partner": 6, "recv1": 5, "recv2": 5}
WIDE = 512

BUFFERS = {
    "far": (2, (2, 2), BF16),
    "near": (6, (2, 2), BF16),
    "partner": (AHEAD["partner"], (2, 2, 2), BF16),
    "send1": (3, (2, 2), BF16),
    "recv1": (AHEAD["recv1"], (2, 2), BF16),
    "send2": (3, (2,), BF16),
    "recv2": (AHEAD["recv2"], (2,), BF16),
    "w_in": (2, (2,), BF16),
    "m_in": (2, (2,), F32),
    "v_in": (2, (2,), F32),
}
SEMS = {"far": 6, "near": 6, "sent1": 3, "recv1": 5, "recv2": 5, "sent2": 3, "ag1": 4, "ag2": 6, "ag3": 7, "sent3": 4}


def adamw(w, m, v, g):
    m = 0.9 * m + 0.1 * g
    v = 0.95 * v + 0.05 * g * g
    step = m * lax.rsqrt(v + 1e-8) + 0.1 * w
    return (w - 0.02 * step).astype(BF16), m, v


def kernel(*refs):
    g, w, m, v = (refs[i : i + 3] for i in (0, 3, 6, 9))
    new_w, new_m, new_v = (refs[i : i + 3] for i in (12, 15, 18))
    own_apart = refs[21]
    refs = list(refs[22:])
    widths = sorted({one.shape[2] for one in m})
    buf = {cols: {name: refs.pop(0) for name in BUFFERS} for cols in widths}
    sem = {name: refs.pop(0) for name in SEMS}
    credit = refs.pop(0)

    spans, total, done = [], 0, dict.fromkeys(widths, 0)
    for i, start, end, parts in RUNS:
        rows, cols = m[i].shape[1:]
        n = rows // CHUNK[cols]
        a, b = n * start // parts, n * end // parts
        spans.append((i, total, total + b - a, a, done[cols]))
        total += b - a
        done[cols] += b - a

    me = lax.axis_index("dp")
    x, y, core = me // 4, (me // 2) % 2, me % 2
    near_x, near_y, partner = me + 4 - 8 * x, me + 2 - 4 * y, me + 1 - 2 * core
    first, second = (near_x, near_y), (near_y, near_x)

    barrier = pltpu.get_barrier_semaphore()
    for other in (partner, near_x, near_y):
        pl.semaphore_signal(barrier, inc=1, device_id={"dp": other}, device_id_type=MESH)
    pl.semaphore_wait(barrier, 3)

    def block(layer, f, s, c):
        fx, fy = (f, s) if layer == 0 else (s, f)
        return (x + fx - 2 * x * fx) * 4 + (y + fy - 2 * y * fy) * 2 + c

    def give(u, name, others):
        @pl.when(u + AHEAD[name] < total)
        def _():
            for k, other in others:
                pl.semaphore_signal(credit.at[k], inc=1, device_id={"dp": other}, device_id_type=MESH)

    def spend(u, name, ks):
        @pl.when(u >= AHEAD[name])
        def _():
            for k in ks:
                pl.semaphore_wait(credit.at[k], 1)

    def run(stage, i, j, u, pos, apart):
        rows, cols = m[i].shape[1:]
        b = buf[cols]
        wide = WIDE if cols % WIDE == 0 else cols
        tall = CHUNK[cols]

        def at(layer, f, s, c=core):
            return (layer, pl.ds(pl.multiple_of(block(layer, f, s, c) * rows + j * tall, tall), tall))

        def of(name):
            return b[name].at[lax.rem(pos, b[name].shape[0])]

        def signal(name):
            return sem[name].at[lax.rem(u, sem[name].shape[0])]

        def take(name, chunks):
            like = g[i].at[0, pl.ds(0, chunks * tall)]
            pltpu.make_async_copy(like, like, signal(name)).wait()

        def local(src, dst, name):
            pltpu.make_async_copy(src, dst, signal(name)).start()

        def remote(src, dst, sent, received, other):
            pltpu.make_async_remote_copy(
                src_ref=src, dst_ref=dst, send_sem=signal(sent), recv_sem=signal(received),
                device_id={"dp": other}, device_id_type=MESH,
            ).start()

        def pieces(body):
            def one(k, _):
                body((slice(None), pl.ds(pl.multiple_of(k * wide, 128), wide)))
                return 0

            lax.fori_loop(0, cols // wide, one, 0)

        own = pl.ds(pl.multiple_of(j * tall, tall), tall)
        other = of("partner")

        if stage == LOAD:
            spend(u, "partner", (0,))
            for side, mine in ((1, "far"), (0, "near")):
                for layer in (0, 1):
                    for s in (0, 1):
                        remote(g[i].at[at(layer, side, s, 1 - core)], other.at[1 - side, layer, s], "sent1", mine, partner)
                for layer in (0, 1):
                    for s in (0, 1):
                        local(g[i].at[at(layer, side, s)], of(mine).at[layer, s], mine)

        if stage == RS1:
            far, out = of("far"), of("send1")
            take("far", 8)
            for layer in (0, 1):
                for s in (0, 1):
                    def add(p, layer=layer, s=s):
                        out[(layer, s, *p)] = (far[(layer, s, *p)].astype(F32) + other[(0, layer, s, *p)].astype(F32)).astype(BF16)
                    pieces(add)
            spend(u, "recv1", (1, 2))
            for layer in (0, 1):
                remote(out.at[layer], of("recv1").at[layer], "sent1", "recv1", first[layer])

        if stage == RS2:
            near, came, out = of("near"), of("recv1"), of("send2")
            take("near", 8)
            take("recv1", 4)
            for layer in (0, 1):
                def add(p, layer=layer):
                    out[(layer, *p)] = (
                        near[(layer, 1, *p)].astype(F32) + other[(1, layer, 1, *p)].astype(F32) + came[(layer, 1, *p)].astype(F32)
                    ).astype(BF16)
                pieces(add)
            take("sent1", 12)
            for layer in (0, 1):
                remote(out.at[layer], of("recv2").at[layer], "sent2", "recv2", second[layer])

        if stage == FETCH:
            for layer in (0, 1):
                local(w[i].at[at(layer, 0, 0)], of("w_in").at[layer], "recv2")
                local(m[i].at[layer, own], of("m_in").at[layer], "recv2")
                local(v[i].at[layer, own], of("v_in").at[layer], "recv2")

        if stage == STEP:
            near, came, last = of("near"), of("recv1"), of("recv2")
            w_in, m_in, v_in = of("w_in"), of("m_in"), of("v_in")
            take("recv2", 12)
            for layer in (0, 1):
                rows_of = at(layer, 0, 0)[1]

                def step(p, layer=layer, rows_of=rows_of):
                    gsum = near[(layer, 0, *p)].astype(F32) + other[(1, layer, 0, *p)].astype(F32)
                    gsum = gsum + came[(layer, 0, *p)].astype(F32) + last[(layer, *p)].astype(F32)
                    gsum = gsum.astype(BF16).astype(F32)
                    one = adamw(w_in[(layer, *p)].astype(F32), m_in[(layer, *p)], v_in[(layer, *p)], gsum)
                    if apart:
                        own_apart[layer, pl.ds(pl.multiple_of((j - SOONER) * tall, tall), tall), p[1]] = one[0]
                    else:
                        new_w[i][layer, rows_of, p[1]] = one[0]
                    new_m[i][layer, own, p[1]] = one[1]
                    new_v[i][layer, own, p[1]] = one[2]
                pieces(step)
            take("sent2", 2)
            give(u, "partner", ((0, partner),))
            give(u, "recv1", ((1, near_x), (2, near_y)))
            for layer in (0, 1):
                if apart:
                    continue
                mine = new_w[i].at[at(layer, 0, 0)]
                remote(mine, mine, "sent3", "ag1", second[layer])
                remote(mine, mine, "sent3", "ag2", first[layer])
                remote(mine, mine, "sent3", "ag3", partner)

        if stage == AG1 and not apart:
            take("ag1", 2)
            for layer in (0, 1):
                came = new_w[i].at[at(layer, 0, 1)]
                remote(came, came, "sent3", "ag2", first[layer])
            for layer in (0, 1):
                came = new_w[i].at[at(layer, 0, 1)]
                remote(came, came, "sent3", "ag3", partner)

        if stage == AG2 and not apart:
            take("ag2", 4)

            @pl.when(u < total - 1)
            def _():
                for layer in (0, 1):
                    for s in (0, 1):
                        came = new_w[i].at[at(layer, 1, s)]
                        remote(came, came, "sent3", "ag3", partner)

        if stage == END and not apart:
            @pl.when(u < total - 1)
            def _():
                take("ag3", 8)
                take("sent3", 14)

            @pl.when(u == total - 1)
            def _():
                take("ag3", 4)
                take("sent3", 10)

    def body(t, _):
        for stage in ORDER:
            u = t - LAG[stage]
            for i, start, end, chunk, pos in spans:
                @pl.when(jnp.logical_and(u >= start, u < end))
                def _(i=i, start=start, chunk=chunk, pos=pos, stage=stage, u=u):
                    run(stage, i, u - start + chunk, u, u - start + pos, i == APART and chunk >= SOONER)
        return 0

    lax.fori_loop(0, total + LAG[END], body, 0)


def far_last(up, layer, s, x, y, core):
    fx, fy = ((1 - x), (1 - y if s else y)) if layer == 0 else ((1 - x if s else x), (1 - y))
    tall, rows = CHUNK[up.shape[2]], up.shape[1] // 8
    start = (fx * 4 + fy * 2 + core) * rows + (SOONER - 1) * tall
    return up.at[layer, pl.ds(pl.multiple_of(start, tall), tall)]


def finish(own, from_x, from_y, up, whole, extra, hop, across, sent, sent_across, across_extra, sent_extra):
    rows, cols = own.shape[1:]
    tall = CHUNK[cols]
    parts = rows // tall
    me = lax.axis_index("dp")
    x, y, core = me // 4, (me // 2) % 2, me % 2
    near_x, near_y, partner = me + 4 - 8 * x, me + 2 - 4 * y, me + 1 - 2 * core
    corner = (1 - x) * 4 + (1 - y) * 2 + core

    barrier = pltpu.get_barrier_semaphore()
    for other in (partner, near_x, near_y):
        pl.semaphore_signal(barrier, inc=1, device_id={"dp": other}, device_id_type=MESH)
    pl.semaphore_wait(barrier, 3)

    def place(layer, device, k, count):
        return whole.at[layer, pl.ds(pl.multiple_of(device * rows + k * tall, tall), count * tall)]

    def remote(src, dst, sent, received, other):
        pltpu.make_async_remote_copy(
            src_ref=src, dst_ref=dst, send_sem=sent, recv_sem=received, device_id={"dp": other}, device_id_type=MESH
        ).start()

    def take(sem, chunks):
        like = whole.at[0, pl.ds(0, chunks * tall)]
        pltpu.make_async_copy(like, like, sem).wait()

    for k in range(parts):
        for layer, came, device, other in ((0, from_y, near_y, near_x), (1, from_x, near_x, near_y)):
            remote(came.at[layer, pl.ds(k * tall, tall)], place(layer, device, k, 1), sent, hop.at[k], other)
    for layer in (0, 1):
        for s in (0, 1):
            remote(far_last(up, layer, s, x, y, core), extra.at[layer, s], sent_extra, across_extra, partner)
    for layer in (0, 1):
        for src, device in ((own, me), (from_x, near_x), (from_y, near_y)):
            remote(src.at[layer], place(layer, device, 0, parts), sent_across, across, partner)
            pltpu.make_async_copy(src.at[layer], place(layer, device, 0, parts), hop.at[parts]).start()
    for k in range(parts):
        take(hop.at[k], 2)
        for layer in (0, 1):
            here = place(layer, corner, k, 1)
            remote(here, here, sent_across, across, partner)
    take(hop.at[parts], 6 * parts)
    take(across, 8 * parts)
    take(sent, 2 * parts)
    take(sent_across, 8 * parts)
    take(across_extra, 4)
    take(sent_extra, 4)


def run_copies(copies):
    for copy in copies:
        copy.start()
    for copy in copies:
        copy.wait()


def copy_whole(n, *refs):
    run_copies([
        pltpu.make_async_copy(src.at[layer], dst.at[layer], refs[2 * n])
        for src, dst in zip(refs[:n], refs[n : 2 * n], strict=True) for layer in (0, 1)
    ])


def copy_sooner(down, up, new_down, new_up, sem):
    run_copies(
        [pltpu.make_async_copy(down.at[layer], new_down.at[layer], sem) for layer in (0, 1)]
        + [pltpu.make_async_copy(up.at[at], new_up.at[at], sem) for at in sooner_and_later(up.shape[1] // 8)[0]]
    )


def copy_later(_, piece, extra, new_up, sem):
    _, later = sooner_and_later(new_up.shape[1] // 8)
    me = lax.axis_index("dp")
    x, y, core = me // 4, (me // 2) % 2, me % 2
    run_copies(
        [pltpu.make_async_copy(piece.at[src], new_up.at[dst], sem) for src, dst in later]
        + [pltpu.make_async_copy(extra.at[layer, s], far_last(new_up, layer, s, x, y, 1 - core), sem) for layer in (0, 1) for s in (0, 1)]
    )


def sooner_and_later(rows):
    first = SOONER * CHUNK[2560]
    rest = rows - first
    each = [(layer, block) for layer in (0, 1) for block in range(8)]
    return (
        [(layer, pl.ds(block * rows, first)) for layer, block in each],
        [((layer, pl.ds(block * rest, rest)), (layer, pl.ds(block * rows + first, rest))) for layer, block in each],
    )


def plain(body, arrays, like, **more):
    return pl.pallas_call(
        body,
        out_shape=tuple(jax.ShapeDtypeStruct(a.shape, a.dtype) for a in like),
        in_specs=[pl.BlockSpec(memory_space=pl.ANY)] * len(arrays),
        out_specs=(pl.BlockSpec(memory_space=pl.ANY),) * len(like),
        scratch_shapes=[pltpu.SemaphoreType.DMA],
        cost_estimate=pl.CostEstimate(flops=10**8, bytes_accessed=2 * 10**7, transcendentals=0),
        compiler_params=pltpu.CompilerParams(vmem_limit_bytes=2**20),
        **more,
    )(*arrays)


def solution(mesh):
    def step(*arrays):
        terms, weights, m, v = (arrays[i : i + 3] for i in (0, 3, 6, 9))
        widths = sorted({one.shape[2] for one in m})
        scratch = [pltpu.VMEM((slots, *held, CHUNK[cols], cols), kind) for cols in widths for slots, held, kind in BUFFERS.values()]
        sems = [pltpu.SemaphoreType.DMA((slots,)) for slots in SEMS.values()]
        rows, cols = m[APART].shape[1:]
        left = rows - SOONER * CHUNK[cols]
        out = pl.pallas_call(
            kernel,
            out_shape=(*(pltpu.VMEM(one.shape, one.dtype) for one in (*weights, *m, *v)), pltpu.VMEM((2, left, cols), BF16)),
            in_specs=[pl.BlockSpec(memory_space=pl.ANY)] * 12,
            out_specs=(pl.BlockSpec(memory_space=pltpu.VMEM),) * 10,
            scratch_shapes=[*scratch, *sems, pltpu.SemaphoreType.REGULAR((3,))],
            compiler_params=pltpu.CompilerParams(collective_id=0, has_side_effects=True, vmem_limit_bytes=int(23 * 2**20)),
        )(*(t[0] for t in terms), *weights, *m, *v)
        gate, up, down, *moments, own = out
        from_x, from_y = (lax.ppermute(own, "dp", [(d, d ^ flip) for d in range(8)]) for flip in (4, 2))
        gate, *moments = plain(functools.partial(copy_whole, 7), (gate, *moments), (gate, *moments))
        down, new_up = plain(copy_sooner, (down, up), (down, up))
        piece, extra = pl.pallas_call(
            finish,
            out_shape=(pltpu.VMEM((2, 8 * left, cols), BF16), pltpu.VMEM((2, 2, CHUNK[cols], cols), BF16)),
            in_specs=[pl.BlockSpec(memory_space=pl.ANY)] * 4,
            out_specs=(pl.BlockSpec(memory_space=pltpu.VMEM),) * 2,
            scratch_shapes=[pltpu.SemaphoreType.DMA((left // CHUNK[cols] + 1,))] + [pltpu.SemaphoreType.DMA] * 5,
            compiler_params=pltpu.CompilerParams(collective_id=1, has_side_effects=True, vmem_limit_bytes=2**20),
        )(own, from_x, from_y, up)
        (up,) = plain(copy_later, (new_up, piece, extra), (new_up,), input_output_aliases={0: 0})
        return (gate, up, down, *moments)

    all_of, cut = P(None, None, None), P(None, "dp", None)
    return jax.shard_map(
        step,
        mesh=mesh,
        in_specs=(P(("rep", "dp"), None, None, None),) * 3 + (all_of,) * 3 + (cut,) * 6,
        out_specs=(P("rep", None, None),) * 3 + (P("rep", "dp", None),) * 6,
        check_vma=False,
    )
```

```python
import functools

import jax
import jax.numpy as jnp
from jax import lax
from jax.experimental import pallas as pl
from jax.experimental.pallas import tpu as pltpu
from jax.sharding import PartitionSpec as P

MESH = pl.DeviceIdType.MESH
F32, BF16 = jnp.float32, jnp.bfloat16

LOAD, RS1, RS2, FETCH, STEP, AG1, AG2, END = range(8)
LAG = (0, 1, 2, 3, 4, 5, 6, 7)
ORDER = (END, RS1, LOAD, RS2, FETCH, STEP, AG1, AG2)
RUNS = ((2, 0, 1, 1), (1, 3, 7, 7), (0, 0, 1, 1), (1, 0, 3, 7))
APART, SOONER = 1, 3
CHUNK = {2560: 16, 896: 32}
AHEAD = {"partner": 6, "recv1": 5, "recv2": 5}
WIDE = 512

BUFFERS = {
    "far": (2, (2, 2), BF16),
    "near": (6, (2, 2), BF16),
    "partner": (AHEAD["partner"], (2, 2, 2), BF16),
    "send1": (3, (2, 2), BF16),
    "recv1": (AHEAD["recv1"], (2, 2), BF16),
    "send2": (3, (2,), BF16),
    "recv2": (AHEAD["recv2"], (2,), BF16),
    "w_in": (2, (2,), BF16),
    "m_in": (2, (2,), F32),
    "v_in": (2, (2,), F32),
}
SEMS = {"far": 6, "near": 6, "sent1": 3, "recv1": 5, "recv2": 5, "sent2": 3, "ag1": 4, "ag2": 6, "ag3": 7, "sent3": 3}


def adamw(w, m, v, g):
    m = 0.9 * m + 0.1 * g
    v = 0.95 * v + 0.05 * g * g
    step = m * lax.rsqrt(v + 1e-8) + 0.1 * w
    return (w - 0.02 * step).astype(BF16), m, v


def kernel(*refs):
    g, w, m, v = (refs[i : i + 3] for i in (0, 3, 6, 9))
    new_w, new_m, new_v = (refs[i : i + 3] for i in (12, 15, 18))
    own_apart = refs[21]
    refs = list(refs[22:])
    widths = sorted({one.shape[2] for one in m})
    buf = {cols: {name: refs.pop(0) for name in BUFFERS} for cols in widths}
    sem = {name: refs.pop(0) for name in SEMS}
    credit = refs.pop(0)

    spans, total, done = [], 0, dict.fromkeys(widths, 0)
    for i, start, end, parts in RUNS:
        rows, cols = m[i].shape[1:]
        n = rows // CHUNK[cols]
        a, b = n * start // parts, n * end // parts
        spans.append((i, total, total + b - a, a, done[cols]))
        total += b - a
        done[cols] += b - a

    me = lax.axis_index("dp")
    x, y, core = me // 4, (me // 2) % 2, me % 2
    near_x, near_y, partner = me + 4 - 8 * x, me + 2 - 4 * y, me + 1 - 2 * core
    first, second = (near_x, near_y), (near_y, near_x)

    barrier = pltpu.get_barrier_semaphore()
    for other in (partner, near_x, near_y):
        pl.semaphore_signal(barrier, inc=1, device_id={"dp": other}, device_id_type=MESH)
    pl.semaphore_wait(barrier, 3)

    def block(layer, f, s, c):
        fx, fy = (f, s) if layer == 0 else (s, f)
        return (x + fx - 2 * x * fx) * 4 + (y + fy - 2 * y * fy) * 2 + c

    def give(u, name, others):
        @pl.when(u + AHEAD[name] < total)
        def _():
            for k, other in others:
                pl.semaphore_signal(credit.at[k], inc=1, device_id={"dp": other}, device_id_type=MESH)

    def spend(u, name, ks):
        @pl.when(u >= AHEAD[name])
        def _():
            for k in ks:
                pl.semaphore_wait(credit.at[k], 1)

    def run(stage, i, j, u, pos, apart):
        rows, cols = m[i].shape[1:]
        b = buf[cols]
        wide = WIDE if cols % WIDE == 0 else cols
        tall = CHUNK[cols]

        def at(layer, f, s, c=core):
            return (layer, pl.ds(pl.multiple_of(block(layer, f, s, c) * rows + j * tall, tall), tall))

        def of(name):
            return b[name].at[lax.rem(pos, b[name].shape[0])]

        def signal(name):
            return sem[name].at[lax.rem(u, sem[name].shape[0])]

        def take(name, chunks):
            like = g[i].at[0, pl.ds(0, chunks * tall)]
            pltpu.make_async_copy(like, like, signal(name)).wait()

        def local(src, dst, name):
            pltpu.make_async_copy(src, dst, signal(name)).start()

        def remote(src, dst, sent, received, other):
            pltpu.make_async_remote_copy(
                src_ref=src, dst_ref=dst, send_sem=signal(sent), recv_sem=signal(received),
                device_id={"dp": other}, device_id_type=MESH,
            ).start()

        def pieces(body):
            def one(k, _):
                body((slice(None), pl.ds(pl.multiple_of(k * wide, 128), wide)))
                return 0

            lax.fori_loop(0, cols // wide, one, 0)

        own = pl.ds(pl.multiple_of(j * tall, tall), tall)
        other = of("partner")

        if stage == LOAD:
            spend(u, "partner", (0,))
            for side, mine in ((1, "far"), (0, "near")):
                for layer in (0, 1):
                    for s in (0, 1):
                        remote(g[i].at[at(layer, side, s, 1 - core)], other.at[1 - side, layer, s], "sent1", mine, partner)
                for layer in (0, 1):
                    for s in (0, 1):
                        local(g[i].at[at(layer, side, s)], of(mine).at[layer, s], mine)

        if stage == RS1:
            far, out = of("far"), of("send1")
            take("far", 8)
            for layer in (0, 1):
                for s in (0, 1):
                    def add(p, layer=layer, s=s):
                        out[(layer, s, *p)] = (far[(layer, s, *p)].astype(F32) + other[(0, layer, s, *p)].astype(F32)).astype(BF16)
                    pieces(add)
            spend(u, "recv1", (1, 2))
            for layer in (0, 1):
                remote(out.at[layer], of("recv1").at[layer], "sent1", "recv1", first[layer])

        if stage == RS2:
            near, came, out = of("near"), of("recv1"), of("send2")
            take("near", 8)
            take("recv1", 4)
            for layer in (0, 1):
                def add(p, layer=layer):
                    out[(layer, *p)] = (
                        near[(layer, 1, *p)].astype(F32) + other[(1, layer, 1, *p)].astype(F32) + came[(layer, 1, *p)].astype(F32)
                    ).astype(BF16)
                pieces(add)
            take("sent1", 12)
            for layer in (0, 1):
                remote(out.at[layer], of("recv2").at[layer], "sent2", "recv2", second[layer])

        if stage == FETCH:
            for layer in (0, 1):
                local(w[i].at[at(layer, 0, 0)], of("w_in").at[layer], "recv2")
                local(m[i].at[layer, own], of("m_in").at[layer], "recv2")
                local(v[i].at[layer, own], of("v_in").at[layer], "recv2")

        if stage == STEP:
            near, came, last = of("near"), of("recv1"), of("recv2")
            w_in, m_in, v_in = of("w_in"), of("m_in"), of("v_in")
            take("recv2", 12)
            for layer in (0, 1):
                rows_of = at(layer, 0, 0)[1]

                def step(p, layer=layer, rows_of=rows_of):
                    gsum = near[(layer, 0, *p)].astype(F32) + other[(1, layer, 0, *p)].astype(F32)
                    gsum = gsum + came[(layer, 0, *p)].astype(F32) + last[(layer, *p)].astype(F32)
                    gsum = gsum.astype(BF16).astype(F32)
                    one = adamw(w_in[(layer, *p)].astype(F32), m_in[(layer, *p)], v_in[(layer, *p)], gsum)
                    if apart:
                        own_apart[layer, pl.ds(pl.multiple_of((j - SOONER) * tall, tall), tall), p[1]] = one[0]
                    else:
                        new_w[i][layer, rows_of, p[1]] = one[0]
                    new_m[i][layer, own, p[1]] = one[1]
                    new_v[i][layer, own, p[1]] = one[2]
                pieces(step)
            take("sent2", 2)
            give(u, "partner", ((0, partner),))
            give(u, "recv1", ((1, near_x), (2, near_y)))
            for layer in (0, 1):
                if apart:
                    continue
                mine = new_w[i].at[at(layer, 0, 0)]
                remote(mine, mine, "sent3", "ag1", second[layer])
                remote(mine, mine, "sent3", "ag2", first[layer])
                remote(mine, mine, "sent3", "ag3", partner)

        if stage == AG1 and not apart:
            take("ag1", 2)
            for layer in (0, 1):
                came = new_w[i].at[at(layer, 0, 1)]
                remote(came, came, "sent3", "ag2", first[layer])
            for layer in (0, 1):
                came = new_w[i].at[at(layer, 0, 1)]
                remote(came, came, "sent3", "ag3", partner)

        if stage == AG2 and not apart:
            take("ag2", 4)

            @pl.when(u < total - 1)
            def _():
                for layer in (0, 1):
                    for s in (0, 1):
                        came = new_w[i].at[at(layer, 1, s)]
                        remote(came, came, "sent3", "ag3", partner)

        if stage == END and not apart:
            @pl.when(u < total - 1)
            def _():
                take("ag3", 8)
                take("sent3", 14)

            @pl.when(u == total - 1)
            def _():
                take("ag3", 4)
                take("sent3", 10)

    def body(t, _):
        for stage in ORDER:
            u = t - LAG[stage]
            for i, start, end, chunk, pos in spans:
                @pl.when(jnp.logical_and(u >= start, u < end))
                def _(i=i, start=start, chunk=chunk, pos=pos, stage=stage, u=u):
                    run(stage, i, u - start + chunk, u, u - start + pos, i == APART and chunk >= SOONER)
        return 0

    lax.fori_loop(0, total + LAG[END], body, 0)


def far_last(up, layer, s, x, y, core):
    fx, fy = ((1 - x), (1 - y if s else y)) if layer == 0 else ((1 - x if s else x), (1 - y))
    tall, rows = CHUNK[up.shape[2]], up.shape[1] // 8
    start = (fx * 4 + fy * 2 + core) * rows + (SOONER - 1) * tall
    return up.at[layer, pl.ds(pl.multiple_of(start, tall), tall)]


def finish(own, from_x, from_y, up, whole, extra, hop, across, sent, sent_across, across_extra, sent_extra):
    rows, cols = own.shape[1:]
    tall = CHUNK[cols]
    parts = rows // tall
    me = lax.axis_index("dp")
    x, y, core = me // 4, (me // 2) % 2, me % 2
    near_x, near_y, partner = me + 4 - 8 * x, me + 2 - 4 * y, me + 1 - 2 * core
    corner = (1 - x) * 4 + (1 - y) * 2 + core

    barrier = pltpu.get_barrier_semaphore()
    for other in (partner, near_x, near_y):
        pl.semaphore_signal(barrier, inc=1, device_id={"dp": other}, device_id_type=MESH)
    pl.semaphore_wait(barrier, 3)

    def place(layer, device, k, count):
        return whole.at[layer, pl.ds(pl.multiple_of(device * rows + k * tall, tall), count * tall)]

    def remote(src, dst, sent, received, other):
        pltpu.make_async_remote_copy(
            src_ref=src, dst_ref=dst, send_sem=sent, recv_sem=received, device_id={"dp": other}, device_id_type=MESH
        ).start()

    def take(sem, chunks):
        like = whole.at[0, pl.ds(0, chunks * tall)]
        pltpu.make_async_copy(like, like, sem).wait()

    for k in range(parts):
        for layer, came, device, other in ((0, from_y, near_y, near_x), (1, from_x, near_x, near_y)):
            remote(came.at[layer, pl.ds(k * tall, tall)], place(layer, device, k, 1), sent, hop.at[k], other)
    for layer in (0, 1):
        for s in (0, 1):
            remote(far_last(up, layer, s, x, y, core), extra.at[layer, s], sent_extra, across_extra, partner)
    for layer in (0, 1):
        for src, device in ((own, me), (from_x, near_x), (from_y, near_y)):
            remote(src.at[layer], place(layer, device, 0, parts), sent_across, across, partner)
            pltpu.make_async_copy(src.at[layer], place(layer, device, 0, parts), hop.at[parts]).start()
    for k in range(parts):
        take(hop.at[k], 2)
        for layer in (0, 1):
            here = place(layer, corner, k, 1)
            remote(here, here, sent_across, across, partner)
    take(hop.at[parts], 6 * parts)
    take(across, 8 * parts)
    take(sent, 2 * parts)
    take(sent_across, 8 * parts)
    take(across_extra, 4)
    take(sent_extra, 4)


def run_copies(copies):
    for copy in copies:
        copy.start()
    for copy in copies:
        copy.wait()


def copy_whole(n, *refs):
    run_copies([
        pltpu.make_async_copy(src.at[layer], dst.at[layer], refs[2 * n])
        for src, dst in zip(refs[:n], refs[n : 2 * n], strict=True) for layer in (0, 1)
    ])


def copy_sooner(down, up, new_down, new_up, sem):
    run_copies(
        [pltpu.make_async_copy(down.at[layer], new_down.at[layer], sem) for layer in (0, 1)]
        + [pltpu.make_async_copy(up.at[at], new_up.at[at], sem) for at in sooner_and_later(up.shape[1] // 8)[0]]
    )


def copy_later(_, piece, extra, new_up, sem):
    _, later = sooner_and_later(new_up.shape[1] // 8)
    me = lax.axis_index("dp")
    x, y, core = me // 4, (me // 2) % 2, me % 2
    run_copies(
        [pltpu.make_async_copy(piece.at[src], new_up.at[dst], sem) for src, dst in later]
        + [pltpu.make_async_copy(extra.at[layer, s], far_last(new_up, layer, s, x, y, 1 - core), sem) for layer in (0, 1) for s in (0, 1)]
    )


def sooner_and_later(rows):
    first = SOONER * CHUNK[2560]
    rest = rows - first
    each = [(layer, block) for layer in (0, 1) for block in range(8)]
    return (
        [(layer, pl.ds(block * rows, first)) for layer, block in each],
        [((layer, pl.ds(block * rest, rest)), (layer, pl.ds(block * rows + first, rest))) for layer, block in each],
    )


def plain(body, arrays, like, **more):
    return pl.pallas_call(
        body,
        out_shape=tuple(jax.ShapeDtypeStruct(a.shape, a.dtype) for a in like),
        in_specs=[pl.BlockSpec(memory_space=pl.ANY)] * len(arrays),
        out_specs=(pl.BlockSpec(memory_space=pl.ANY),) * len(like),
        scratch_shapes=[pltpu.SemaphoreType.DMA],
        cost_estimate=pl.CostEstimate(flops=10**8, bytes_accessed=2 * 10**7, transcendentals=0),
        compiler_params=pltpu.CompilerParams(vmem_limit_bytes=2**20),
        **more,
    )(*arrays)


def solution(mesh):
    def step(*arrays):
        terms, weights, m, v = (arrays[i : i + 3] for i in (0, 3, 6, 9))
        widths = sorted({one.shape[2] for one in m})
        scratch = [pltpu.VMEM((slots, *held, CHUNK[cols], cols), kind) for cols in widths for slots, held, kind in BUFFERS.values()]
        sems = [pltpu.SemaphoreType.DMA((slots,)) for slots in SEMS.values()]
        rows, cols = m[APART].shape[1:]
        left = rows - SOONER * CHUNK[cols]
        out = pl.pallas_call(
            kernel,
            out_shape=(*(pltpu.VMEM(one.shape, one.dtype) for one in (*weights, *m, *v)), pltpu.VMEM((2, left, cols), BF16)),
            in_specs=[pl.BlockSpec(memory_space=pl.ANY)] * 12,
            out_specs=(pl.BlockSpec(memory_space=pltpu.VMEM),) * 10,
            scratch_shapes=[*scratch, *sems, pltpu.SemaphoreType.REGULAR((3,))],
            compiler_params=pltpu.CompilerParams(collective_id=0, has_side_effects=True, vmem_limit_bytes=int(23 * 2**20)),
        )(*(t[0] for t in terms), *weights, *m, *v)
        gate, up, down, *moments, own = out
        from_x, from_y = (lax.ppermute(own, "dp", [(d, d ^ flip) for d in range(8)]) for flip in (4, 2))
        gate, *moments = plain(functools.partial(copy_whole, 7), (gate, *moments), (gate, *moments))
        down, new_up = plain(copy_sooner, (down, up), (down, up))
        piece, extra = pl.pallas_call(
            finish,
            out_shape=(pltpu.VMEM((2, 8 * left, cols), BF16), pltpu.VMEM((2, 2, CHUNK[cols], cols), BF16)),
            in_specs=[pl.BlockSpec(memory_space=pl.ANY)] * 4,
            out_specs=(pl.BlockSpec(memory_space=pltpu.VMEM),) * 2,
            scratch_shapes=[pltpu.SemaphoreType.DMA((left // CHUNK[cols] + 1,))] + [pltpu.SemaphoreType.DMA] * 5,
            compiler_params=pltpu.CompilerParams(collective_id=1, has_side_effects=True, vmem_limit_bytes=2**20),
        )(own, from_x, from_y, up)
        (up,) = plain(copy_later, (new_up, piece, extra), (new_up,), input_output_aliases={0: 0})
        return (gate, up, down, *moments)

    all_of, cut = P(None, None, None), P(None, "dp", None)
    return jax.shard_map(
        step,
        mesh=mesh,
        in_specs=(P(("rep", "dp"), None, None, None),) * 3 + (all_of,) * 3 + (cut,) * 6,
        out_specs=(P("rep", None, None),) * 3 + (P("rep", "dp", None),) * 6,
        check_vma=False,
    )
```
